128 devices in a mesh: dp: 8 (over x, core), tensor: 16 (over z, y).
Axes of the slice: x: 4, y: 4, z: 4, core: 2. Of those that a mesh axis runs over, the one named last changes fastest.
Arguments:
- attn_ctx: bfloat16 [4096, 8192], P('dp', 'tensor'), may hold values from -6 to 6
- w_out: bfloat16 [8192, 8192], P('tensor'), may hold values from -0.09375 to 0.09375
- resid: bfloat16 [4096, 8192], P(('dp', 'tensor')), may hold values from -6 to 6
- teacher_gain: bfloat16 [8192], replicated, may hold values from 0.25 to 1.75
- dest_row: int32 [4096], replicated, may hold values from 0 to 4095, as said below
- student_in: bfloat16 [4096, 4096], P('dp', 'tensor'), may hold values from -6 to 6
- student_gain: bfloat16 [4096], replicated, may hold values from 0.25 to 1.75
- w_gate: bfloat16 [4096, 14336], P('dp', 'tensor'), may hold values from -0.09375 to 0.09375
- w_up: bfloat16 [4096, 14336], P('dp', 'tensor'), may hold values from -0.09375 to 0.09375
- w_down: bfloat16 [14336, 4096], P('tensor', 'dp'), may hold values from -0.0625 to 0.0625
- proj: bfloat16 [4096, 8192], P('dp', 'tensor'), may hold values from -0.09375 to 0.09375
Outputs:
- student_out: bfloat16 [4096, 4096], P('dp', 'tensor')
- row_loss: float32 [4096], P('dp')
- residue: float32 [4096, 8192], P('dp', 'tensor')
The draws below stay inside these ranges and needn't reach their ends.
Inputs may be any that keep to these rules, and one draw needn't show every extreme that they name: A permutation of the rows; of the 32 rows i in one aligned block of teacher rows, at most 8 have dest_row[i] in any one tile of 512 student rows, and some tile receives exactly 8 of them.
All inputs are finite; a program needn't handle non-finite values.
Results may differ from the reference program's by a relative error of at most 0.012.
Values may be sent and summed in bfloat16 or wider, within the bound.
A program may use at most 128 MiB of HBM per device.

```python
import jax
import jax.numpy as jnp
from jax import lax

HT = 8192
D = 4096
FF = 14336
TT = 512
TOKENS = 4096
N_DP = 8
N_TENSOR = 16


def draw_dest_row(key, part):
    rows_dev = TT // N_TENSOR
    mean_count = rows_dev // N_DP
    sources = N_DP * N_TENSOR
    keys = jax.random.split(jax.random.fold_in(key, 7), 5)
    amounts = jax.random.randint(keys[0], (N_DP // 2,), 0, mean_count + 1)
    amounts = amounts.at[0].set(mean_count)
    counts = jnp.stack([mean_count + amounts, mean_count - amounts], 1).reshape(N_DP)
    counts = counts[jax.random.permutation(keys[1], N_DP)]
    rotation = jax.random.permutation(keys[2], sources) % N_DP
    shifted = (jnp.arange(N_DP)[None, :] + rotation[:, None]) % N_DP
    per_source = counts[shifted]
    bounds = jnp.cumsum(per_source, 1)
    position = jnp.arange(rows_dev)
    labels = jnp.sum((position[None, :, None] >= bounds[:, None, :]).astype(jnp.int32), 2)
    orders = jax.vmap(lambda one_key: jax.random.permutation(one_key, rows_dev))(jax.random.split(keys[3], sources))
    labels = jnp.take_along_axis(labels, orders, 1).reshape(-1)
    onehot = (labels[:, None] == jnp.arange(N_DP)[None, :]).astype(jnp.int32)
    ranking = jnp.sum((jnp.cumsum(onehot, 0) - onehot) * onehot, 1)
    placing = jax.vmap(lambda one_key: jax.random.permutation(one_key, TT))(jax.random.split(keys[4], N_DP))
    return (labels * TT + placing[labels, ranking]).astype(jnp.int32)


def with_spikes(drawn, stream_key, source, target, parts, factor):
    def block_of(axis_at):
        return (jnp.arange(drawn.shape[axis_at]) // (drawn.shape[axis_at] // parts)).reshape((-1,) + (1,) * (drawn.ndim - 1 - axis_at))

    near = jax.random.permutation(stream_key, parts)[block_of(target)]
    far = (block_of(target) + parts // 2) % parts
    return jnp.where((block_of(source) == near) | (block_of(source) == far), factor * drawn, drawn)


def level_of(stream_key, shape, cuts, least, high):
    factor_of = 1.0
    for dim, blocks in cuts:
        heights = jax.random.uniform(jax.random.fold_in(jax.random.fold_in(stream_key, 6), dim), (blocks,), jnp.float32, least / len(cuts), high / len(cuts))
        factor_of = factor_of * jnp.repeat(jnp.exp(heights), shape[dim] // blocks).reshape((-1,) + (1,) * (len(shape) - 1 - dim))
    return factor_of


def scatter_about(own_key, extent, scale, bound, cuts=(), kind=jnp.bfloat16):
    values = jax.random.normal(own_key, extent, jnp.float32) * scale
    if len(cuts) > 0:
        values = level_of(own_key, extent, cuts, -0.22, 0.18) * values
    return jnp.clip(values, min=-bound, max=bound).astype(kind)


def gaussian_with(key, shape, width, bound, cuts, heavy, dtype=jnp.bfloat16):
    values = width * jax.random.normal(key, shape, jnp.float32)
    if cuts:
        values = values * level_of(key, shape, cuts, -0.22, 0.18)
    return jnp.clip(with_spikes(values, jax.random.fold_in(key, 3), *heavy), -bound, bound).astype(dtype)


def setup_inputs(seed: int = 0) -> dict:
    splits = jax.random.split(jax.random.key(seed), 12)
    attn_ctx = scatter_about(splits[0], (TOKENS, HT), 1.0, 6.0, ((0, 8), (1, 16)))
    w_out = gaussian_with(splits[1], (HT, HT), HT ** -0.5, 0.09375, ((0, 16),), (0, 1, 16, 2.0))
    resid = scatter_about(splits[2], (TOKENS, HT), 1.0, 6.0, ((0, 128),))
    teacher_gain = jnp.clip(1.0 + 0.15 * jax.random.normal(splits[3], (HT,), jnp.float32), 0.25, 1.75).astype(jnp.bfloat16)
    dest_row = draw_dest_row(jax.random.fold_in(splits[11], 71), 0)
    student_in = scatter_about(splits[5], (TOKENS, D), 1.0, 6.0, ((0, 8), (1, 16)))
    student_gain = jnp.clip(1.0 + 0.15 * jax.random.normal(splits[6], (D,), jnp.float32), 0.25, 1.75).astype(jnp.bfloat16)
    w_gate = scatter_about(splits[7], (D, FF), D ** -0.5, 0.09375, ((0, 8), (1, 16)))
    w_up = scatter_about(splits[8], (D, FF), D ** -0.5, 0.09375, ((0, 8), (1, 16)))
    w_down = gaussian_with(splits[9], (FF, D), FF ** -0.5, 0.0625, ((0, 16), (1, 8)), (0, 1, 16, 2.0))
    proj = scatter_about(splits[10], (D, HT), D ** -0.5, 0.09375, ((0, 8), (1, 16)))
    return dict(attn_ctx=attn_ctx, w_out=w_out, resid=resid, teacher_gain=teacher_gain, dest_row=dest_row, student_in=student_in, student_gain=student_gain, w_gate=w_gate, w_up=w_up, w_down=w_down, proj=proj)


def reference(attn_ctx, w_out, resid, teacher_gain, dest_row, student_in, student_gain, w_gate, w_up, w_down, proj):
    blocks_ctx = attn_ctx.reshape(TOKENS, N_TENSOR, HT // N_TENSOR).transpose(1, 0, 2)
    blocks_out = w_out.reshape(N_TENSOR, HT // N_TENSOR, HT)

    def add_term(running, pair):
        term = jnp.dot(pair[0], pair[1], preferred_element_type=jnp.float32)
        term = lax.optimization_barrier(term.astype(jnp.bfloat16)).astype(jnp.float32)
        return (running + term, None)
    attn_sum, unused = lax.scan(add_term, jnp.zeros((TOKENS, HT), jnp.float32), (blocks_ctx, blocks_out))
    teacher_hidden = resid.astype(jnp.float32) + attn_sum
    square_mean = lax.optimization_barrier(jnp.mean(teacher_hidden * teacher_hidden, axis=1, keepdims=True))
    teacher_final = (teacher_hidden * lax.rsqrt(square_mean + 1e-06) * teacher_gain.astype(jnp.float32)).astype(jnp.bfloat16)
    target = jnp.zeros((TOKENS, HT), jnp.bfloat16).at[dest_row].set(teacher_final)
    x_full = student_in.astype(jnp.float32)
    student_mean = lax.optimization_barrier(jnp.mean(x_full * x_full, axis=1, keepdims=True))
    normed = (x_full * lax.rsqrt(student_mean + 1e-05) * student_gain.astype(jnp.float32)).astype(jnp.bfloat16)
    gate_acts = jnp.dot(normed, w_gate, preferred_element_type=jnp.float32)
    up_acts = jnp.dot(normed, w_up, preferred_element_type=jnp.float32)
    hidden = (jax.nn.silu(gate_acts) * up_acts).astype(jnp.bfloat16)
    mlp_sum = jnp.dot(hidden, w_down, preferred_element_type=jnp.float32)
    student_out = (x_full + mlp_sum).astype(jnp.bfloat16)
    pred = jnp.dot(student_out, proj, preferred_element_type=jnp.float32)
    residue = pred - target.astype(jnp.float32)
    row_loss = lax.optimization_barrier(jnp.mean(residue * residue, axis=1))
    return (student_out, row_loss, residue)
```

```python
import functools
import jax
import jax.numpy as jnp
from jax import lax
from jax.sharding import Mesh
from jax.sharding import PartitionSpec as P
from jax.experimental import pallas as pl
from jax.experimental.pallas import tpu as pltpu

HT = 8192
BF = jnp.bfloat16
F32 = jnp.float32
AXES = ("x", "c", "z", "y")
TENSOR = ("z", "y")
DP = ("x", "c")


class Net:
    def __init__(self, send_sems, recv_sems):
        self.ss, self.rs, self.made = send_sems, recv_sems, {}

    def send(self, role, src, dst, dev):
        i = len(self.made)
        cp = pltpu.make_async_remote_copy(
            src_ref=src,
            dst_ref=dst,
            send_sem=self.ss.at[i],
            recv_sem=self.rs.at[i],
            device_id=dev,
            device_id_type=pl.DeviceIdType.MESH,
        )
        cp.start()
        self.made[role] = cp

    def got(self, *roles):
        for role in roles:
            self.made[role].wait_recv()

    def drain(self):
        for cp in self.made.values():
            cp.wait_send()


def greet(partners):
    barrier = pltpu.get_barrier_semaphore()
    for dev in partners:
        pl.semaphore_signal(barrier, inc=1, device_id=dev, device_id_type=pl.DeviceIdType.MESH)
    pl.semaphore_wait(barrier, len(partners))


N1 = 68


def first_kernel(
    attn, wout_hbm, resid, sin, gain, wg_hbm, wu_hbm,
    hid, th, xrow,
    w1, xg, nrm, wout, part, rp, rq, sp, sq, rp2, rq2, acc, tmp, loc, wsem, ss, rs,
):
    x, c, z, y = (lax.axis_index(a) for a in AXES)
    t = z * 4 + y
    d = x * 2 + c

    def at(base, k):
        return lax.rem(base + k, 4)

    xr, xl, xo = at(x, 1), at(x, 3), at(x, 2)
    sib = {"c": 1 - c}
    right, left = {"x": xr}, {"x": xl}
    loads = []
    for h in range(2):
        rows = pl.ds(h * 256, 256)
        loads.append(pltpu.make_async_copy(wg_hbm.at[rows], w1.at[d, h, :, pl.ds(0, 896)], loc.at[2 * h]))
        loads.append(pltpu.make_async_copy(wu_hbm.at[rows], w1.at[d, h, :, pl.ds(896, 896)], loc.at[2 * h + 1]))
    loads.append(pltpu.make_async_copy(sin, xg.at[z, y], loc.at[4]))
    for cp in loads:
        cp.start()
    wloads = [
        pltpu.make_async_copy(wout_hbm.at[:, pl.ds(b * 512, 512)], wout.at[b], wsem.at[b]) for b in range(16)
    ]
    for cp in wloads:
        cp.start()

    greet(
        [sib, right, left]
        + [{"y": at(y, k)} for k in (1, 2, 3)]
        + [{"z": at(z, k)} for k in (1, 2, 3)]
    )
    net = Net(ss, rs)

    def piece(who, half):
        return pl.ds(who * 256 + half * 128, 128)

    def ring_open(tag, axis, base, ref):
        up, down = {axis: at(base, 1)}, {axis: at(base, 3)}
        net.send(tag + "LA", ref(0, 0), ref(0, 0), up)
        net.send(tag + "RB", ref(0, 1), ref(0, 1), down)
        net.send(tag + "LB", ref(0, 1), ref(0, 1), up)
        net.send(tag + "RA", ref(0, 0), ref(0, 0), down)

    def ring_forward(tag, axis, base, ref):
        up, down = {axis: at(base, 1)}, {axis: at(base, 3)}
        net.got(tag + "LA")
        net.send(tag + "OA", ref(3, 0), ref(3, 0), up)
        net.got(tag + "RB")
        net.send(tag + "OB", ref(1, 1), ref(1, 1), down)

    def ring_close(tag):
        net.got(tag + "LB", tag + "RA", tag + "OA", tag + "OB")

    p1 = lambda k, h: xg.at[z, at(y, k), piece(0, h)]
    q1 = lambda k, h: xg.at[at(z, k), y, piece(1, h)]
    p2 = lambda k, h: xg.at[at(z, k), :, piece(0, h)]
    q2 = lambda k, h: xg.at[:, at(y, k), piece(1, h)]

    loads[4].wait()
    ring_open("p1", "y", y, p1)
    ring_open("q1", "z", z, q1)
    for cp in loads[:4]:
        cp.wait()
    net.send("wLA", w1.at[d, 0], w1.at[d, 0], right)
    net.send("wRB", w1.at[d, 1], w1.at[d, 1], left)
    net.send("wLB", w1.at[d, 1], w1.at[d, 1], right)
    net.send("wRA", w1.at[d, 0], w1.at[d, 0], left)
    net.send("sIA", w1.at[d, 0], w1.at[d, 0], sib)
    net.send("sIB", w1.at[d, 1], w1.at[d, 1], sib)

    mine = pl.ds(pl.multiple_of(t * 32, 32), 32)

    def partial(b):
        wloads[b].wait()
        tmp[...] = jnp.dot(attn[...], wout[b], preferred_element_type=F32)
        tmp[mine, :] += resid[:, b * 512:(b + 1) * 512].astype(F32)
        part[b] = tmp[...].astype(BF)

    partial(0)
    partial(1)
    partial(2)
    partial(3)
    ring_forward("p1", "y", y, p1)
    ring_forward("q1", "z", z, q1)
    partial(4)
    partial(5)
    ring_close("p1")
    ring_open("p2", "z", z, p2)
    ring_close("q1")
    ring_open("q2", "y", y, q2)
    for b in range(6, 16):
        partial(b)
    ring_forward("p2", "z", z, p2)
    ring_forward("q2", "y", y, q2)

    P_ROWS, Q_ROWS = pl.ds(0, 256), pl.ds(256, 256)
    for k in (1, 2, 3, 0):
        for j in (1, 2, 3):
            zz, yy = at(z, k), at(y, j)
            net.send(f"tp{k}{j}", part.at[zz * 4 + yy, P_ROWS], rp.at[j - 1, k], {"y": yy})
            zz, yy = at(z, j), at(y, k)
            net.send(f"tq{k}{j}", part.at[zz * 4 + yy, Q_ROWS], rq.at[j - 1, k], {"z": zz})

    ring_close("p2")
    ring_close("q2")
    xrow[...] = xg[:, :, mine, :].reshape(16, 32, 256)

    @pl.loop(0, 4)
    def _(r):
        rows = pl.ds(pl.multiple_of(r * 128, 128), 128)
        total = jnp.zeros((128, 256), F32)
        for s in range(16):
            v = xg[s // 4, s % 4, rows, :].astype(F32)
            total = total + v * v
        scale = lax.rsqrt(jnp.sum(total, axis=1, keepdims=True) / 4096.0 + 1e-05)
        for s in range(16):
            v = xg[s // 4, s % 4, rows, :].astype(F32)
            nrm[s, rows, :] = (v * scale * gain[s:s + 1, :].astype(F32)).astype(BF)

    def gate_up(slots, first):
        @pl.loop(0, 7)
        def _(j):
            cols = pl.ds(pl.multiple_of(j * 256, 256), 256)
            total = None
            for s, h in slots:
                term = jnp.dot(nrm[s * 2 + h], w1[s, h, :, cols], preferred_element_type=F32)
                total = term if total is None else total + term
            if first:
                acc[:, cols] = total
            else:
                acc[:, cols] += total

    def slot(xx, cc):
        return xx * 2 + cc

    def pass_on(role, s, h):
        net.send(role, w1.at[s, h], w1.at[s, h], sib)

    net.got("wLA")
    net.send("wOA", w1.at[slot(xl, c), 0], w1.at[slot(xl, c), 0], right)
    pass_on("sLA", slot(xl, c), 0)
    net.got("wRB")
    net.send("wOB", w1.at[slot(xr, c), 1], w1.at[slot(xr, c), 1], left)
    pass_on("sRB", slot(xr, c), 1)
    net.got("sIA", "sIB")
    gate_up([(d, 0), (d, 1), (slot(x, 1 - c), 0), (slot(x, 1 - c), 1)], True)
    net.got("sLA", "sRB")
    gate_up([(slot(xl, c), 0), (slot(xr, c), 1), (slot(xl, 1 - c), 0), (slot(xr, 1 - c), 1)], False)

    def reduce_p(k):
        net.got(f"tp{k}1", f"tp{k}2", f"tp{k}3")
        zz = at(z, k)
        s = part[zz * 4 + y, :256, :].astype(F32)
        for j in range(3):
            s = s + rp[j, k].astype(F32)
        if k == 0:
            th[:256, :] = s
        else:
            sp[k - 1] = s.astype(BF)
            net.send(f"up{k}", sp.at[k - 1], rp2.at[k - 1], {"z": zz})

    def reduce_q(k):
        net.got(f"tq{k}1", f"tq{k}2", f"tq{k}3")
        yy = at(y, k)
        s = part[z * 4 + yy, 256:, :].astype(F32)
        for j in range(3):
            s = s + rq[j, k].astype(F32)
        if k == 0:
            th[256:, :] = s
        else:
            sq[k - 1] = s.astype(BF)
            net.send(f"uq{k}", sq.at[k - 1], rq2.at[k - 1], {"y": yy})

    reduce_p(1)
    reduce_q(1)
    net.got("wLB")
    pass_on("sLB", slot(xl, c), 1)
    net.got("wRA")
    pass_on("sRA", slot(xr, c), 0)
    net.got("sLB", "sRA")
    gate_up([(slot(xl, c), 1), (slot(xr, c), 0), (slot(xl, 1 - c), 1), (slot(xr, 1 - c), 0)], False)
    reduce_p(2)
    reduce_q(2)
    net.got("wOA")
    pass_on("sOA", slot(xo, c), 0)
    net.got("wOB")
    pass_on("sOB", slot(xo, c), 1)
    reduce_p(3)
    reduce_q(3)
    net.got("sOA", "sOB")
    gate_up([(slot(xo, c), 0), (slot(xo, c), 1), (slot(xo, 1 - c), 0), (slot(xo, 1 - c), 1)], False)

    @pl.loop(0, 7)
    def _(j):
        g = acc[:, pl.ds(pl.multiple_of(j * 128, 128), 128)]
        u = acc[:, pl.ds(pl.multiple_of(896 + j * 128, 128), 128)]
        hid[:, pl.ds(pl.multiple_of(j * 128, 128), 128)] = (jax.nn.silu(g) * u).astype(BF)

    reduce_p(0)
    reduce_q(0)
    for k in (1, 2, 3):
        net.got(f"up{k}")
        th[:256, :] += rp2[k - 1].astype(F32)
        net.got(f"uq{k}")
        th[256:, :] += rq2[k - 1].astype(F32)
    net.drain()


def call_first(attn, wout, resid, sin, gain, wg, wu):
    vm = pl.BlockSpec(memory_space=pltpu.VMEM)
    hb = pl.BlockSpec(memory_space=pl.ANY)
    return pl.pallas_call(
        first_kernel,
        name="first",
        out_shape=(
            jax.ShapeDtypeStruct((512, 896), BF),
            jax.ShapeDtypeStruct((512, 512), F32),
            jax.ShapeDtypeStruct((16, 32, 256), BF),
        ),
        in_specs=[vm, hb, vm, vm, vm, hb, hb],
        out_specs=(vm, vm, vm),
        scratch_shapes=[
            pltpu.VMEM((8, 2, 256, 1792), BF),
            pltpu.VMEM((4, 4, 512, 256), BF),
            pltpu.VMEM((16, 512, 256), BF),
            pltpu.VMEM((16, 512, 512), BF),
            pltpu.VMEM((16, 512, 512), BF),
            pltpu.VMEM((3, 4, 256, 512), BF),
            pltpu.VMEM((3, 4, 256, 512), BF),
            pltpu.VMEM((3, 256, 512), BF),
            pltpu.VMEM((3, 256, 512), BF),
            pltpu.VMEM((3, 256, 512), BF),
            pltpu.VMEM((3, 256, 512), BF),
            pltpu.VMEM((512, 1792), F32),
            pltpu.VMEM((512, 512), F32),
            pltpu.SemaphoreType.DMA((5,)),
            pltpu.SemaphoreType.DMA((16,)),
            pltpu.SemaphoreType.DMA((N1,)),
            pltpu.SemaphoreType.DMA((N1,)),
        ],
        compiler_params=pltpu.CompilerParams(
            collective_id=0, has_side_effects=True, vmem_limit_bytes=67043328
        ),
    )(attn, wout, resid, sin, gain, wg, wu)


def one_axis_at_a_time(value, axes):
    for axis in axes:
        value = lax.psum(value, axis)
    return value


def local(
    attn_ctx,
    w_out,
    resid,
    teacher_gain,
    dest_row,
    student_in,
    student_gain,
    w_gate,
    w_up,
    w_down,
    proj,
):
    t = lax.axis_index(TENSOR)
    d = lax.axis_index(DP)
    hidden, th, xrow = call_first(
        attn_ctx, w_out, resid, student_in, student_gain.reshape(16, 256), w_gate, w_up
    )
    ssq = lax.psum(jnp.sum(th * th, axis=1), TENSOR)
    gain = lax.dynamic_slice_in_dim(teacher_gain, t * 512, 512, 0).astype(F32)
    final = (th * lax.rsqrt(ssq / HT + 1e-06)[:, None] * gain[None, :]).astype(BF)
    everyone = lax.all_gather(final, DP, axis=0, tiled=True)
    pick = (dest_row[None, :] == (d * 512 + jnp.arange(512))[:, None]).astype(BF)
    target = jnp.dot(pick, everyone, preferred_element_type=F32)
    partial_sum = jnp.dot(
        hidden, lax.all_gather(w_down, DP, axis=1, tiled=True), preferred_element_type=F32
    )
    rows = lax.psum_scatter(partial_sum.astype(BF), TENSOR, scatter_dimension=0, tiled=True).astype(F32)
    out_rows = (rows + xrow.transpose(1, 0, 2).reshape(32, 4096).astype(F32)).astype(BF)
    out_full = lax.all_gather(out_rows, TENSOR, axis=0, tiled=True)
    out_local = lax.dynamic_slice_in_dim(out_full, t * 256, 256, 1)
    pred = jnp.dot(
        out_full, lax.all_gather(proj, DP, axis=0, tiled=True), preferred_element_type=F32
    )
    residue = pred - target
    row_loss = one_axis_at_a_time(jnp.sum(residue * residue, axis=1), TENSOR) / HT
    return (out_local, row_loss, residue)


def solution(mesh):
    torus = Mesh(mesh.devices.reshape(4, 2, 4, 4), AXES)
    in_specs = (
        P(DP, TENSOR),
        P(TENSOR, None),
        P(DP + TENSOR, None),
        P(),
        P(),
        P(DP, TENSOR),
        P(),
        P(DP, TENSOR),
        P(DP, TENSOR),
        P(TENSOR, DP),
        P(DP, TENSOR),
    )
    out_specs = (P(DP, TENSOR), P(DP), P(DP, TENSOR))
    return jax.shard_map(local, mesh=torus, in_specs=in_specs, out_specs=out_specs, check_vma=False)
```

```python
import functools
import jax
import jax.numpy as jnp
from jax import lax
from jax.sharding import Mesh
from jax.sharding import PartitionSpec as P
from jax.experimental import pallas as pl
from jax.experimental.pallas import tpu as pltpu

HT = 8192
BF = jnp.bfloat16
F32 = jnp.float32
AXES = ("x", "c", "z", "y")
TENSOR = ("z", "y")
DP = ("x", "c")


class Net:
    def __init__(self, send_sems, recv_sems):
        self.ss, self.rs, self.made = send_sems, recv_sems, {}

    def send(self, role, src, dst, dev):
        i = len(self.made)
        cp = pltpu.make_async_remote_copy(
            src_ref=src,
            dst_ref=dst,
            send_sem=self.ss.at[i],
            recv_sem=self.rs.at[i],
            device_id=dev,
            device_id_type=pl.DeviceIdType.MESH,
        )
        cp.start()
        self.made[role] = cp

    def got(self, *roles):
        for role in roles:
            self.made[role].wait_recv()

    def drain(self):
        for cp in self.made.values():
            cp.wait_send()


def greet(partners):
    barrier = pltpu.get_barrier_semaphore()
    for dev in partners:
        pl.semaphore_signal(barrier, inc=1, device_id=dev, device_id_type=pl.DeviceIdType.MESH)
    pl.semaphore_wait(barrier, len(partners))


N1 = 68


def first_kernel(
    attn, wout_hbm, resid, sin, gain, wg_hbm, wu_hbm,
    hid, th, xrow,
    w1, xg, nrm, wout, part, rp, rq, sp, sq, rp2, rq2, acc, tmp, loc, wsem, ss, rs,
):
    x, c, z, y = (lax.axis_index(a) for a in AXES)
    t = z * 4 + y
    d = x * 2 + c

    def at(base, k):
        return lax.rem(base + k, 4)

    xr, xl, xo = at(x, 1), at(x, 3), at(x, 2)
    sib = {"c": 1 - c}
    right, left = {"x": xr}, {"x": xl}
    loads = []
    for h in range(2):
        rows = pl.ds(h * 256, 256)
        loads.append(pltpu.make_async_copy(wg_hbm.at[rows], w1.at[d, h, :, pl.ds(0, 896)], loc.at[2 * h]))
        loads.append(pltpu.make_async_copy(wu_hbm.at[rows], w1.at[d, h, :, pl.ds(896, 896)], loc.at[2 * h + 1]))
    loads.append(pltpu.make_async_copy(sin, xg.at[z, y], loc.at[4]))
    for cp in loads:
        cp.start()
    wloads = [
        pltpu.make_async_copy(wout_hbm.at[:, pl.ds(b * 512, 512)], wout.at[b], wsem.at[b]) for b in range(16)
    ]
    for cp in wloads:
        cp.start()

    greet(
        [sib, right, left]
        + [{"y": at(y, k)} for k in (1, 2, 3)]
        + [{"z": at(z, k)} for k in (1, 2, 3)]
    )
    net = Net(ss, rs)

    def piece(who, half):
        return pl.ds(who * 256 + half * 128, 128)

    def ring_open(tag, axis, base, ref):
        up, down = {axis: at(base, 1)}, {axis: at(base, 3)}
        net.send(tag + "LA", ref(0, 0), ref(0, 0), up)
        net.send(tag + "RB", ref(0, 1), ref(0, 1), down)
        net.send(tag + "LB", ref(0, 1), ref(0, 1), up)
        net.send(tag + "RA", ref(0, 0), ref(0, 0), down)

    def ring_forward(tag, axis, base, ref):
        up, down = {axis: at(base, 1)}, {axis: at(base, 3)}
        net.got(tag + "LA")
        net.send(tag + "OA", ref(3, 0), ref(3, 0), up)
        net.got(tag + "RB")
        net.send(tag + "OB", ref(1, 1), ref(1, 1), down)

    def ring_close(tag):
        net.got(tag + "LB", tag + "RA", tag + "OA", tag + "OB")

    p1 = lambda k, h: xg.at[z, at(y, k), piece(0, h)]
    q1 = lambda k, h: xg.at[at(z, k), y, piece(1, h)]
    p2 = lambda k, h: xg.at[at(z, k), :, piece(0, h)]
    q2 = lambda k, h: xg.at[:, at(y, k), piece(1, h)]

    loads[4].wait()
    ring_open("p1", "y", y, p1)
    ring_open("q1", "z", z, q1)
    for cp in loads[:4]:
        cp.wait()
    net.send("wLA", w1.at[d, 0], w1.at[d, 0], right)
    net.send("wRB", w1.at[d, 1], w1.at[d, 1], left)
    net.send("wLB", w1.at[d, 1], w1.at[d, 1], right)
    net.send("wRA", w1.at[d, 0], w1.at[d, 0], left)
    net.send("sIA", w1.at[d, 0], w1.at[d, 0], sib)
    net.send("sIB", w1.at[d, 1], w1.at[d, 1], sib)

    mine = pl.ds(pl.multiple_of(t * 32, 32), 32)

    def partial(b):
        wloads[b].wait()
        tmp[...] = jnp.dot(attn[...], wout[b], preferred_element_type=F32)
        tmp[mine, :] += resid[:, b * 512:(b + 1) * 512].astype(F32)
        part[b] = tmp[...].astype(BF)

    partial(0)
    partial(1)
    partial(2)
    partial(3)
    ring_forward("p1", "y", y, p1)
    ring_forward("q1", "z", z, q1)
    partial(4)
    partial(5)
    ring_close("p1")
    ring_open("p2", "z", z, p2)
    ring_close("q1")
    ring_open("q2", "y", y, q2)
    for b in range(6, 16):
        partial(b)
    ring_forward("p2", "z", z, p2)
    ring_forward("q2", "y", y, q2)

    P_ROWS, Q_ROWS = pl.ds(0, 256), pl.ds(256, 256)
    for k in (1, 2, 3, 0):
        for j in (1, 2, 3):
            zz, yy = at(z, k), at(y, j)
            net.send(f"tp{k}{j}", part.at[zz * 4 + yy, P_ROWS], rp.at[j - 1, k], {"y": yy})
            zz, yy = at(z, j), at(y, k)
            net.send(f"tq{k}{j}", part.at[zz * 4 + yy, Q_ROWS], rq.at[j - 1, k], {"z": zz})

    ring_close("p2")
    ring_close("q2")
    xrow[...] = xg[:, :, mine, :].reshape(16, 32, 256)

    @pl.loop(0, 4)
    def _(r):
        rows = pl.ds(pl.multiple_of(r * 128, 128), 128)
        total = jnp.zeros((128, 256), F32)
        for s in range(16):
            v = xg[s // 4, s % 4, rows, :].astype(F32)
            total = total + v * v
        scale = lax.rsqrt(jnp.sum(total, axis=1, keepdims=True) / 4096.0 + 1e-05)
        for s in range(16):
            v = xg[s // 4, s % 4, rows, :].astype(F32)
            nrm[s, rows, :] = (v * scale * gain[s:s + 1, :].astype(F32)).astype(BF)

    def gate_up(slots, first):
        @pl.loop(0, 7)
        def _(j):
            cols = pl.ds(pl.multiple_of(j * 256, 256), 256)
            total = None
            for s, h in slots:
                term = jnp.dot(nrm[s * 2 + h], w1[s, h, :, cols], preferred_element_type=F32)
                total = term if total is None else total + term
            if first:
                acc[:, cols] = total
            else:
                acc[:, cols] += total

    def slot(xx, cc):
        return xx * 2 + cc

    def pass_on(role, s, h):
        net.send(role, w1.at[s, h], w1.at[s, h], sib)

    net.got("wLA")
    net.send("wOA", w1.at[slot(xl, c), 0], w1.at[slot(xl, c), 0], right)
    pass_on("sLA", slot(xl, c), 0)
    net.got("wRB")
    net.send("wOB", w1.at[slot(xr, c), 1], w1.at[slot(xr, c), 1], left)
    pass_on("sRB", slot(xr, c), 1)
    net.got("sIA", "sIB")
    gate_up([(d, 0), (d, 1), (slot(x, 1 - c), 0), (slot(x, 1 - c), 1)], True)
    net.got("sLA", "sRB")
    gate_up([(slot(xl, c), 0), (slot(xr, c), 1), (slot(xl, 1 - c), 0), (slot(xr, 1 - c), 1)], False)

    def reduce_p(k):
        net.got(f"tp{k}1", f"tp{k}2", f"tp{k}3")
        zz = at(z, k)
        s = part[zz * 4 + y, :256, :].astype(F32)
        for j in range(3):
            s = s + rp[j, k].astype(F32)
        if k == 0:
            th[:256, :] = s
        else:
            sp[k - 1] = s.astype(BF)
            net.send(f"up{k}", sp.at[k - 1], rp2.at[k - 1], {"z": zz})

    def reduce_q(k):
        net.got(f"tq{k}1", f"tq{k}2", f"tq{k}3")
        yy = at(y, k)
        s = part[z * 4 + yy, 256:, :].astype(F32)
        for j in range(3):
            s = s + rq[j, k].astype(F32)
        if k == 0:
            th[256:, :] = s
        else:
            sq[k - 1] = s.astype(BF)
            net.send(f"uq{k}", sq.at[k - 1], rq2.at[k - 1], {"y": yy})

    reduce_p(1)
    reduce_q(1)
    net.got("wLB")
    pass_on("sLB", slot(xl, c), 1)
    net.got("wRA")
    pass_on("sRA", slot(xr, c), 0)
    net.got("sLB", "sRA")
    gate_up([(slot(xl, c), 1), (slot(xr, c), 0), (slot(xl, 1 - c), 1), (slot(xr, 1 - c), 0)], False)
    reduce_p(2)
    reduce_q(2)
    net.got("wOA")
    pass_on("sOA", slot(xo, c), 0)
    net.got("wOB")
    pass_on("sOB", slot(xo, c), 1)
    reduce_p(3)
    reduce_q(3)
    net.got("sOA", "sOB")
    gate_up([(slot(xo, c), 0), (slot(xo, c), 1), (slot(xo, 1 - c), 0), (slot(xo, 1 - c), 1)], False)

    @pl.loop(0, 7)
    def _(j):
        g = acc[:, pl.ds(pl.multiple_of(j * 128, 128), 128)]
        u = acc[:, pl.ds(pl.multiple_of(896 + j * 128, 128), 128)]
        hid[:, pl.ds(pl.multiple_of(j * 128, 128), 128)] = (jax.nn.silu(g) * u).astype(BF)

    reduce_p(0)
    reduce_q(0)
    for k in (1, 2, 3):
        net.got(f"up{k}")
        th[:256, :] += rp2[k - 1].astype(F32)
        net.got(f"uq{k}")
        th[256:, :] += rq2[k - 1].astype(F32)
    net.drain()


def call_first(attn, wout, resid, sin, gain, wg, wu):
    vm = pl.BlockSpec(memory_space=pltpu.VMEM)
    hb = pl.BlockSpec(memory_space=pl.ANY)
    return pl.pallas_call(
        first_kernel,
        name="first",
        out_shape=(
            jax.ShapeDtypeStruct((512, 896), BF),
            jax.ShapeDtypeStruct((512, 512), F32),
            jax.ShapeDtypeStruct((16, 32, 256), BF),
        ),
        in_specs=[vm, hb, vm, vm, vm, hb, hb],
        out_specs=(vm, vm, vm),
        scratch_shapes=[
            pltpu.VMEM((8, 2, 256, 1792), BF),
            pltpu.VMEM((4, 4, 512, 256), BF),
            pltpu.VMEM((16, 512, 256), BF),
            pltpu.VMEM((16, 512, 512), BF),
            pltpu.VMEM((16, 512, 512), BF),
            pltpu.VMEM((3, 4, 256, 512), BF),
            pltpu.VMEM((3, 4, 256, 512), BF),
            pltpu.VMEM((3, 256, 512), BF),
            pltpu.VMEM((3, 256, 512), BF),
            pltpu.VMEM((3, 256, 512), BF),
            pltpu.VMEM((3, 256, 512), BF),
            pltpu.VMEM((512, 1792), F32),
            pltpu.VMEM((512, 512), F32),
            pltpu.SemaphoreType.DMA((5,)),
            pltpu.SemaphoreType.DMA((16,)),
            pltpu.SemaphoreType.DMA((N1,)),
            pltpu.SemaphoreType.DMA((N1,)),
        ],
        compiler_params=pltpu.CompilerParams(
            collective_id=0, has_side_effects=True, vmem_limit_bytes=67043328
        ),
    )(attn, wout, resid, sin, gain, wg, wu)


N2 = 174


def second_kernel(
    hid, wd_hbm, pj_hbm, xrow, th, tgain, dest,
    out, res, loss,
    w2, pj, tg, pt, so, r1, s1, r2, stat_y, stat_z, stat_s, loss_y, loss_z, loss_s, loc, ss, rs,
):
    x, c, z, y = (lax.axis_index(a) for a in AXES)
    t = z * 4 + y
    d = x * 2 + c

    def at(base, k):
        return lax.rem(base + k, 4)

    xr, xl, xo = at(x, 1), at(x, 3), at(x, 2)
    sib = {"c": 1 - c}
    right, left = {"x": xr}, {"x": xl}
    w2_loads, pj_loads = [], []
    for h in range(2):
        w2_loads.append(pltpu.make_async_copy(wd_hbm.at[:, pl.ds(h * 256, 256)], w2.at[d, h], loc.at[h]))
        pj_loads.append(pltpu.make_async_copy(pj_hbm.at[pl.ds(h * 256, 256)], pj.at[d, h], loc.at[2 + h]))
    for cp in w2_loads + pj_loads:
        cp.start()
    greet(
        [sib, right, left]
        + [{"y": at(y, k)} for k in (1, 2, 3)]
        + [{"z": at(z, k)} for k in (1, 2, 3)]
    )
    net = Net(ss, rs)
    owner = {"I": x, "L": xl, "R": xr, "O": xo}
    half = {"A": 0, "B": 1}

    def shard(role, core):
        return owner[role[0]] * 2 + core, half[role[1]]

    def along_x_open(tag, buf):
        net.send(tag + "LA", buf.at[d, 0], buf.at[d, 0], right)
        net.send(tag + "RB", buf.at[d, 1], buf.at[d, 1], left)
        net.send(tag + "LB", buf.at[d, 1], buf.at[d, 1], right)
        net.send(tag + "RA", buf.at[d, 0], buf.at[d, 0], left)
        net.send(tag + "sIA", buf.at[d, 0], buf.at[d, 0], sib)
        net.send(tag + "sIB", buf.at[d, 1], buf.at[d, 1], sib)

    def along_x_take(tag, buf, role):
        ref = buf.at[shard(role, c)]
        net.got(tag + role)
        if role == "LA":
            net.send(tag + "OA", ref, ref, right)
        if role == "RB":
            net.send(tag + "OB", ref, ref, left)
        net.send(tag + "s" + role, ref, ref, sib)

    groups = (("IA", "IB"), ("LA", "RB"), ("LB", "RA"), ("OA", "OB"))

    def partial(g, pq):
        core = c if pq == 0 else 1 - c
        for i in range(2):
            term = jnp.dot(hid[...], w2[shard(groups[g][i], core)], preferred_element_type=F32)
            pt[g, pq, :, :, :, i * 256:(i + 1) * 256] = term.astype(BF).reshape(4, 4, 32, 256)
        for j in (1, 2, 3):
            if pq == 0:
                yy = at(y, j)
                net.send(f"a{g}0{j}", pt.at[g, 0, :, yy], r1.at[g, 0, j - 1], {"y": yy})
            else:
                zz = at(z, j)
                net.send(f"a{g}1{j}", pt.at[g, 1, zz], r1.at[g, 1, j - 1], {"z": zz})

    own_sum = {}

    def middle(g, pq):
        net.got(*[f"a{g}{pq}{j}" for j in (1, 2, 3)])
        for k in (1, 2, 3, 0):
            other = at(z if pq == 0 else y, k)
            mine = pt[g, 0, other, y] if pq == 0 else pt[g, 1, z, other]
            s = mine.astype(F32)
            for j in range(3):
                s = s + r1[g, pq, j, other].astype(F32)
            if k == 0:
                own_sum[g, pq] = s
            else:
                s1[g, pq, k - 1] = s.astype(BF)
                dev = {"z": other} if pq == 0 else {"y": other}
                net.send(f"b{g}{pq}{k}", s1.at[g, pq, k - 1], r2.at[g, pq, k - 1], dev)

    def finish(g, pq):
        net.got(*[f"b{g}{pq}{j}" for j in (1, 2, 3)])
        s = own_sum[g, pq]
        for j in range(3):
            s = s + r2[g, pq, j].astype(F32)
        core = c if pq == 0 else 1 - c
        for i in range(2):
            dd, h = shard(groups[g][i], core)
            xin = xrow[dd * 2 + h].astype(F32)
            so[g, pq, z, y, :, i * 256:(i + 1) * 256] = (xin + s[:, i * 256:(i + 1) * 256]).astype(BF)
        ref = so.at[g, pq, z, y]
        for j in (1, 2, 3):
            dev = {"y": at(y, j)} if pq == 0 else {"z": at(z, j)}
            net.send(f"c{g}{pq}{j}", ref, ref, dev)

    def spread_parts(g, pq):
        if pq == 0:
            return "z", z, lambda k, h: so.at[g, 0, at(z, k), pl.ds(2 * h, 2)]
        return "y", y, lambda k, h: so.at[g, 1, pl.ds(2 * h, 2), at(y, k)]

    def spread_open(g, pq):
        net.got(*[f"c{g}{pq}{j}" for j in (1, 2, 3)])
        axis, base, ref = spread_parts(g, pq)
        tag = f"d{g}{pq}"
        up, down = {axis: at(base, 1)}, {axis: at(base, 3)}
        net.send(tag + "LA", ref(0, 0), ref(0, 0), up)
        net.send(tag + "RB", ref(0, 1), ref(0, 1), down)
        net.send(tag + "LB", ref(0, 1), ref(0, 1), up)
        net.send(tag + "RA", ref(0, 0), ref(0, 0), down)

    def spread_forward(g, pq):
        axis, base, ref = spread_parts(g, pq)
        tag = f"d{g}{pq}"
        net.got(tag + "LA")
        net.send(tag + "OA", ref(3, 0), ref(3, 0), {axis: at(base, 1)})
        net.got(tag + "RB")
        net.send(tag + "OB", ref(1, 1), ref(1, 1), {axis: at(base, 3)})

    def spread_close(g, pq):
        tag = f"d{g}{pq}"
        net.got(tag + "LB", tag + "RA", tag + "OA", tag + "OB")

    def predict(g):
        spread_close(g, 0)
        spread_close(g, 1)
        for pq in range(2):
            core = c if pq == 0 else 1 - c
            left_side = so[g, pq].reshape(512, 512)
            total = None
            for i in range(2):
                term = jnp.dot(
                    left_side[:, i * 256:(i + 1) * 256],
                    pj[shard(groups[g][i], core)],
                    preferred_element_type=F32,
                )
                total = term if total is None else total + term
            if g == 0 and pq == 0:
                res[...] = total
            else:
                res[...] += total

    def row_squares(value):
        v = value * value
        v = v[:, 0:128] + v[:, 128:256] + v[:, 256:384] + v[:, 384:512]
        v = v.T
        parts = v[0:8, :]
        for i in range(1, 16):
            parts = parts + v[8 * i:8 * i + 8, :]
        return parts

    def stat_open(tag, own, inbox, axis, base):
        for j in (1, 2, 3):
            net.send(f"{tag}{j}", own, inbox.at[j - 1], {axis: at(base, j)})

    def stat_take(tag, own, inbox):
        net.got(*[f"{tag}{j}" for j in (1, 2, 3)])
        return own[...] + inbox[0] + inbox[1] + inbox[2]

    def landed(g):
        return target_of(groups[g], c) + target_of(groups[g], 1 - c)

    def target_of(roles, core):
        return [shard(r, core) for r in roles]

    row_id = d * 512 + lax.broadcasted_iota(jnp.int32, (512, 256), 0)

    def subtract_target(slots):
        total = None
        for dd, h in slots:
            pick = dest[dd * 2 + h]
            onehot = jnp.where(row_id == pick, 1.0, 0.0).astype(BF)
            term = jnp.dot(onehot, tg[dd, h], preferred_element_type=F32)
            total = term if total is None else total + term
        res[...] -= total

    stat_s[0] = row_squares(th[...])
    stat_open("ty", stat_s.at[0], stat_y, "y", y)
    for cp in w2_loads:
        cp.wait()
    along_x_open("w", w2)
    partial(0, 0)
    stat_s[1] = stat_take("ty", stat_s.at[0], stat_y)
    stat_open("tz", stat_s.at[1], stat_z, "z", z)
    net.got("wsIA", "wsIB")
    partial(0, 1)
    total = jnp.sum(stat_take("tz", stat_s.at[1], stat_z), axis=0, keepdims=True)
    scale = jnp.broadcast_to(lax.rsqrt(total / HT + 1e-06), (128, 512)).T
    gain = tgain[t].astype(F32)
    for h in range(2):
        for i in range(4):
            rows, cols = slice(h * 256, h * 256 + 256), slice(i * 128, i * 128 + 128)
            tg[d, h, :, cols] = (th[rows, cols] * scale[rows, :] * gain[:, cols]).astype(BF)
    middle(0, 0)
    middle(0, 1)
    finish(0, 0)
    finish(0, 1)
    along_x_take("w", w2, "LA")
    along_x_take("w", w2, "RB")
    partial(1, 0)
    spread_open(0, 0)
    spread_open(0, 1)
    net.got("wsLA", "wsRB")
    partial(1, 1)
    for cp in pj_loads:
        cp.wait()
    along_x_open("p", pj)
    middle(1, 0)
    middle(1, 1)
    spread_forward(0, 0)
    spread_forward(0, 1)
    finish(1, 0)
    finish(1, 1)
    along_x_take("w", w2, "LB")
    along_x_take("w", w2, "RA")
    partial(2, 0)
    spread_open(1, 0)
    spread_open(1, 1)
    net.got("wsLB", "wsRA")
    partial(2, 1)
    middle(2, 0)
    middle(2, 1)
    spread_forward(1, 0)
    spread_forward(1, 1)
    finish(2, 0)
    finish(2, 1)
    along_x_take("w", w2, "OA")
    along_x_take("w", w2, "OB")
    partial(3, 0)
    spread_open(2, 0)
    spread_open(2, 1)
    net.got("wsOA", "wsOB")
    partial(3, 1)
    along_x_take("p", pj, "LA")
    along_x_take("p", pj, "RB")
    along_x_open("t", tg)
    middle(3, 0)
    middle(3, 1)
    spread_forward(2, 0)
    spread_forward(2, 1)
    finish(3, 0)
    finish(3, 1)
    net.got("psIA", "psIB")
    predict(0)
    spread_open(3, 0)
    spread_open(3, 1)
    net.got("psLA", "psRB")
    predict(1)
    along_x_take("p", pj, "LB")
    along_x_take("p", pj, "RA")
    spread_forward(3, 0)
    spread_forward(3, 1)
    net.got("psLB", "psRA")
    predict(2)
    along_x_take("p", pj, "OA")
    along_x_take("p", pj, "OB")
    along_x_take("t", tg, "LA")
    along_x_take("t", tg, "RB")
    net.got("tsIA", "tsIB")
    subtract_target(landed(0))
    net.got("psOA", "psOB")
    predict(3)

    h0 = lax.rem(t, 2)
    d0 = lax.div(t, 2)
    k0 = lax.rem(lax.div(d0, 2) - x + 4, 4)
    k_odd, k_two = lax.rem(k0, 2), lax.div(k0, 2)
    g0 = (1 - k_odd) * k_two * 3 + k_odd * (k_two * (1 + h0) + (1 - k_two) * (2 - h0))
    i0 = (1 - k_odd) * h0 + k_odd * (1 - k_two)
    pq0 = lax.rem(d0 + c, 2)
    out[...] = so[g0, pq0, :, :, :, pl.ds(pl.multiple_of(i0 * 256, 256), 256)].reshape(512, 256)

    net.got("tsLA", "tsRB")
    subtract_target(landed(1))
    along_x_take("t", tg, "LB")
    along_x_take("t", tg, "RA")
    net.got("tsLB", "tsRA")
    subtract_target(landed(2))
    along_x_take("t", tg, "OA")
    along_x_take("t", tg, "OB")
    net.got("tsOA", "tsOB")
    subtract_target(landed(3))

    loss_s[0] = row_squares(res[...])
    stat_open("ly", loss_s.at[0], loss_y, "y", y)
    loss_s[1] = stat_take("ly", loss_s.at[0], loss_y)
    stat_open("lz", loss_s.at[1], loss_z, "z", z)
    total = jnp.sum(stat_take("lz", loss_s.at[1], loss_z), axis=0, keepdims=True)
    loss[...] = total / HT
    net.drain()


def call_second(hid, wd, pj, xrow, th, tgain, dest):
    vm = pl.BlockSpec(memory_space=pltpu.VMEM)
    hb = pl.BlockSpec(memory_space=pl.ANY)
    return pl.pallas_call(
        second_kernel,
        name="second",
        out_shape=(
            jax.ShapeDtypeStruct((512, 256), BF),
            jax.ShapeDtypeStruct((512, 512), F32),
            jax.ShapeDtypeStruct((1, 512), F32),
        ),
        in_specs=[vm, hb, hb, vm, vm, vm, vm],
        out_specs=(vm, vm, vm),
        scratch_shapes=[
            pltpu.VMEM((8, 2, 896, 256), BF),
            pltpu.VMEM((8, 2, 256, 512), BF),
            pltpu.VMEM((8, 2, 256, 512), BF),
            pltpu.VMEM((4, 2, 4, 4, 32, 512), BF),
            pltpu.VMEM((4, 2, 4, 4, 32, 512), BF),
            pltpu.VMEM((4, 2, 3, 4, 32, 512), BF),
            pltpu.VMEM((4, 2, 3, 32, 512), BF),
            pltpu.VMEM((4, 2, 3, 32, 512), BF),
            pltpu.VMEM((3, 8, 512), F32),
            pltpu.VMEM((3, 8, 512), F32),
            pltpu.VMEM((2, 8, 512), F32),
            pltpu.VMEM((3, 8, 512), F32),
            pltpu.VMEM((3, 8, 512), F32),
            pltpu.VMEM((2, 8, 512), F32),
            pltpu.SemaphoreType.DMA((4,)),
            pltpu.SemaphoreType.DMA((N2,)),
            pltpu.SemaphoreType.DMA((N2,)),
        ],
        compiler_params=pltpu.CompilerParams(
            collective_id=1, has_side_effects=True, vmem_limit_bytes=67043328
        ),
    )(hid, wd, pj, xrow, th, tgain, dest)


def local(
    attn_ctx,
    w_out,
    resid,
    teacher_gain,
    dest_row,
    student_in,
    student_gain,
    w_gate,
    w_up,
    w_down,
    proj,
):
    hidden, th, xrow = call_first(
        attn_ctx, w_out, resid, student_in, student_gain.reshape(16, 256), w_gate, w_up
    )
    out, residue, loss = call_second(
        hidden, w_down, proj, xrow, th, teacher_gain.reshape(16, 1, 512), dest_row.reshape(16, 1, 256)
    )
    return (out, loss.reshape(512), residue)


def solution(mesh):
    torus = Mesh(mesh.devices.reshape(4, 2, 4, 4), AXES)
    in_specs = (
        P(DP, TENSOR),
        P(TENSOR, None),
        P(DP + TENSOR, None),
        P(),
        P(),
        P(DP, TENSOR),
        P(),
        P(DP, TENSOR),
        P(DP, TENSOR),
        P(TENSOR, DP),
        P(DP, TENSOR),
    )
    out_specs = (P(DP, TENSOR), P(DP), P(DP, TENSOR))
    return jax.shard_map(local, mesh=torus, in_specs=in_specs, out_specs=out_specs, check_vma=False)
```

```python
import functools
import jax
import jax.numpy as jnp
from jax import lax
from jax.sharding import Mesh
from jax.sharding import PartitionSpec as P
from jax.experimental import pallas as pl
from jax.experimental.pallas import tpu as pltpu

HT = 8192
BF = jnp.bfloat16
F32 = jnp.float32
AXES = ("x", "c", "z", "y")
TENSOR = ("z", "y")
DP = ("x", "c")


class Net:
    def __init__(self, send_sems, recv_sems):
        self.ss, self.rs, self.made = send_sems, recv_sems, {}

    def send(self, role, src, dst, dev):
        i = len(self.made)
        cp = pltpu.make_async_remote_copy(
            src_ref=src,
            dst_ref=dst,
            send_sem=self.ss.at[i],
            recv_sem=self.rs.at[i],
            device_id=dev,
            device_id_type=pl.DeviceIdType.MESH,
        )
        cp.start()
        self.made[role] = cp

    def got(self, *roles):
        for role in roles:
            self.made[role].wait_recv()

    def drain(self):
        for cp in self.made.values():
            cp.wait_send()


def greet(partners):
    barrier = pltpu.get_barrier_semaphore()
    for dev in partners:
        pl.semaphore_signal(barrier, inc=1, device_id=dev, device_id_type=pl.DeviceIdType.MESH)
    pl.semaphore_wait(barrier, len(partners))


N1 = 92


def first_kernel(
    attn, wout_hbm, resid, sin, gain, wg_hbm, wu_hbm,
    hid, th, xrow,
    w1, xg, nrm, wout, part, rp, rq, sp, sq, rp2, rq2, acc, tmp, loc, wsem, ss, rs,
):
    x, c, z, y = (lax.axis_index(a) for a in AXES)
    t = z * 4 + y
    d = x * 2 + c

    def at(base, k):
        return lax.rem(base + k, 4)

    xr, xl, xo = at(x, 1), at(x, 3), at(x, 2)
    sib = {"c": 1 - c}
    right, left = {"x": xr}, {"x": xl}
    loads = []
    for h in range(2):
        rows = pl.ds(h * 256, 256)
        loads.append(pltpu.make_async_copy(wg_hbm.at[rows], w1.at[d, h, :, pl.ds(0, 896)], loc.at[2 * h]))
        loads.append(pltpu.make_async_copy(wu_hbm.at[rows], w1.at[d, h, :, pl.ds(896, 896)], loc.at[2 * h + 1]))
    loads.append(pltpu.make_async_copy(sin, xg.at[z, y], loc.at[4]))
    for cp in loads:
        cp.start()

    order = (
        (1, 1), (1, 2), (2, 1), (1, 3), (3, 1), (2, 2), (2, 3), (3, 2), (3, 3),
        (0, 1), (1, 0), (0, 2), (2, 0), (0, 3), (3, 0), (0, 0),
    )

    def block_cols(dz, dy):
        return pl.ds(pl.multiple_of((at(z, dz) * 4 + at(y, dy)) * 512, 512), 512)

    wloads = {
        b: pltpu.make_async_copy(wout_hbm.at[:, block_cols(*b)], wout.at[i], wsem.at[i])
        for i, b in enumerate(order)
    }

    greet(
        [sib, right, left]
        + [{"y": at(y, k)} for k in (1, 2, 3)]
        + [{"z": at(z, k)} for k in (1, 2, 3)]
    )
    net = Net(ss, rs)

    def piece(who, half):
        return pl.ds(who * 256 + half * 128, 128)

    def ring_open(tag, axis, base, ref, src=None):
        up, down = {axis: at(base, 1)}, {axis: at(base, 3)}
        src = src or (lambda h: ref(0, h))
        net.send(tag + "LA", src(0), ref(0, 0), up)
        net.send(tag + "RB", src(1), ref(0, 1), down)
        net.send(tag + "LB", src(1), ref(0, 1), up)
        net.send(tag + "RA", src(0), ref(0, 0), down)

    def ring_forward(tag, axis, base, ref):
        up, down = {axis: at(base, 1)}, {axis: at(base, 3)}
        net.got(tag + "LA")
        net.send(tag + "OA", ref(3, 0), ref(3, 0), up)
        net.got(tag + "RB")
        net.send(tag + "OB", ref(1, 1), ref(1, 1), down)

    def ring_close(tag):
        net.got(tag + "LB", tag + "RA", tag + "OA", tag + "OB")

    p1 = lambda k, h: xg.at[z, at(y, k), piece(0, h)]
    q1 = lambda k, h: xg.at[at(z, k), y, piece(1, h)]
    p2 = lambda k, h: xg.at[at(z, k), :, piece(0, h)]
    q2 = lambda k, h: xg.at[:, at(y, k), piece(1, h)]

    ring_open("p1", "y", y, p1, lambda h: sin.at[piece(0, h)])
    ring_open("q1", "z", z, q1, lambda h: sin.at[piece(1, h)])
    for cp in loads[:4]:
        cp.wait()
    net.send("wLA", w1.at[d, 0], w1.at[d, 0], right)
    net.send("wRB", w1.at[d, 1], w1.at[d, 1], left)
    net.send("wLB", w1.at[d, 1], w1.at[d, 1], right)
    net.send("wRA", w1.at[d, 0], w1.at[d, 0], left)
    for b in order:
        wloads[b].start()
    net.send("sIA", w1.at[d, 0], w1.at[d, 0], sib)
    net.send("sIB", w1.at[d, 1], w1.at[d, 1], sib)

    mine = pl.ds(pl.multiple_of(t * 32, 32), 32)

    def partial(b):
        i = order.index(b)
        wloads[b].wait()
        tmp[...] = jnp.dot(attn[...], wout[i], preferred_element_type=F32)
        tmp[mine, :] += resid[:, block_cols(*b)].astype(F32)
        part[b[0] * 4 + b[1]] = tmp[...].astype(BF)

    def term(pq, k, j, h):
        b = k * 4 + j if pq == 0 else j * 4 + k
        return b, pl.ds(pq * 256 + h * 128, 128)

    def sum_dev(pq, j):
        return {"y": at(y, j)} if pq == 0 else {"z": at(z, j)}

    inbox = (rp, rq)

    def sum_send(name, pq, k, j, h, slot, to):
        b, rows = term(pq, k, j, h)
        net.send(f"{name}{pq}{k}", part.at[b, rows], inbox[pq].at[k, slot], sum_dev(pq, to))

    def sum_open(pq, k):
        sum_send("fA", pq, k, 2, 0, 0, 1)
        sum_send("fB", pq, k, 2, 1, 1, 3)
        sum_send("uB", pq, k, 1, 1, 3, 1)
        sum_send("dA", pq, k, 3, 0, 4, 3)

    def sum_pass(pq, k):
        for name, j, h, slot, out, to in (("fA", 1, 0, 0, "uA", 1), ("fB", 3, 1, 1, "dB", 3)):
            net.got(f"{name}{pq}{k}")
            b, rows = term(pq, k, j, h)
            part[b, rows, :] = (part[b, rows, :].astype(F32) + inbox[pq][k, slot].astype(F32)).astype(BF)
            sum_send(out, pq, k, j, h, 2 if out == "uA" else 5, to)

    def sum_close(pq, k):
        net.got(*[f"{name}{pq}{k}" for name in ("uA", "uB", "dA", "dB")])
        store, box = (sp, rp2) if pq == 0 else (sq, rq2)
        for h in range(2):
            b, rows = term(pq, k, 0, h)
            s = part[b, rows, :].astype(F32)
            s = s + inbox[pq][k, 2 + h].astype(F32) + inbox[pq][k, 4 + h].astype(F32)
            if k == 0:
                th[rows, :] = s
            else:
                store[k - 1, h * 128:h * 128 + 128] = s.astype(BF)
        if k:
            dev = {"z": at(z, k)} if pq == 0 else {"y": at(y, k)}
            net.send(f"v{pq}{k}", store.at[k - 1], box.at[k - 1], dev)

    for b in order[:5]:
        partial(b)
    ring_forward("p1", "y", y, p1)
    ring_forward("q1", "z", z, q1)
    sum_open(0, 1)
    sum_open(1, 1)
    partial(order[5])
    partial(order[6])
    loads[4].wait()
    ring_close("p1")
    ring_open("p2", "z", z, p2)
    ring_close("q1")
    ring_open("q2", "y", y, q2)
    partial(order[7])
    partial(order[8])
    sum_pass(0, 1)
    sum_pass(1, 1)
    for b in order[9:]:
        partial(b)
    sum_open(0, 2)
    sum_open(1, 2)
    ring_forward("p2", "z", z, p2)
    ring_forward("q2", "y", y, q2)
    sum_open(0, 3)
    sum_open(1, 3)

    def gate_up(slots, first):
        @pl.loop(0, 7)
        def _(j):
            cols = pl.ds(pl.multiple_of(j * 256, 256), 256)
            total = None
            for s, h in slots:
                term = jnp.dot(nrm[s * 2 + h], w1[s, h, :, cols], preferred_element_type=F32)
                total = term if total is None else total + term
            if first:
                acc[:, cols] = total
            else:
                acc[:, cols] += total

    def slot(xx, cc):
        return xx * 2 + cc

    def pass_on(role, s, h):
        net.send(role, w1.at[s, h], w1.at[s, h], sib)

    net.got("wLA")
    net.send("wOA", w1.at[slot(xl, c), 0], w1.at[slot(xl, c), 0], right)
    pass_on("sLA", slot(xl, c), 0)
    net.got("wRB")
    net.send("wOB", w1.at[slot(xr, c), 1], w1.at[slot(xr, c), 1], left)
    pass_on("sRB", slot(xr, c), 1)
    sum_pass(0, 2)
    sum_pass(1, 2)
    sum_open(0, 0)
    sum_open(1, 0)

    ring_close("p2")
    ring_close("q2")
    xrow[...] = xg[:, :, mine, :].reshape(16, 32, 256)

    @pl.loop(0, 4)
    def _(r):
        rows = pl.ds(pl.multiple_of(r * 128, 128), 128)
        total = jnp.zeros((128, 256), F32)
        for s in range(16):
            v = xg[s // 4, s % 4, rows, :].astype(F32)
            total = total + v * v
        scale = lax.rsqrt(jnp.sum(total, axis=1, keepdims=True) / 4096.0 + 1e-05)
        for s in range(16):
            v = xg[s // 4, s % 4, rows, :].astype(F32)
            nrm[s, rows, :] = (v * scale * gain[s:s + 1, :].astype(F32)).astype(BF)

    sum_pass(0, 3)
    sum_pass(1, 3)
    net.got("sIA", "sIB")
    gate_up([(d, 0), (d, 1), (slot(x, 1 - c), 0), (slot(x, 1 - c), 1)], True)
    sum_close(0, 1)
    sum_close(1, 1)
    sum_pass(0, 0)
    sum_pass(1, 0)
    net.got("sLA", "sRB")
    gate_up([(slot(xl, c), 0), (slot(xr, c), 1), (slot(xl, 1 - c), 0), (slot(xr, 1 - c), 1)], False)
    net.got("wLB")
    pass_on("sLB", slot(xl, c), 1)
    net.got("wRA")
    pass_on("sRA", slot(xr, c), 0)
    sum_close(0, 2)
    sum_close(1, 2)
    net.got("sLB", "sRA")
    gate_up([(slot(xl, c), 1), (slot(xr, c), 0), (slot(xl, 1 - c), 1), (slot(xr, 1 - c), 0)], False)
    sum_close(0, 3)
    sum_close(1, 3)
    net.got("wOA")
    pass_on("sOA", slot(xo, c), 0)
    net.got("wOB")
    pass_on("sOB", slot(xo, c), 1)
    sum_close(0, 0)
    sum_close(1, 0)
    net.got("sOA", "sOB")
    gate_up([(slot(xo, c), 0), (slot(xo, c), 1), (slot(xo, 1 - c), 0), (slot(xo, 1 - c), 1)], False)

    @pl.loop(0, 7)
    def _(j):
        g = acc[:, pl.ds(pl.multiple_of(j * 128, 128), 128)]
        u = acc[:, pl.ds(pl.multiple_of(896 + j * 128, 128), 128)]
        hid[:, pl.ds(pl.multiple_of(j * 128, 128), 128)] = (jax.nn.silu(g) * u).astype(BF)

    for k in (1, 2, 3):
        net.got(f"v0{k}")
        th[:256, :] += rp2[k - 1].astype(F32)
        net.got(f"v1{k}")
        th[256:, :] += rq2[k - 1].astype(F32)
    net.drain()


def call_first(attn, wout, resid, sin, gain, wg, wu):
    vm = pl.BlockSpec(memory_space=pltpu.VMEM)
    hb = pl.BlockSpec(memory_space=pl.ANY)
    return pl.pallas_call(
        first_kernel,
        name="first",
        out_shape=(
            jax.ShapeDtypeStruct((512, 896), BF),
            jax.ShapeDtypeStruct((512, 512), F32),
            jax.ShapeDtypeStruct((16, 32, 256), BF),
        ),
        in_specs=[vm, hb, vm, vm, vm, hb, hb],
        out_specs=(vm, vm, vm),
        scratch_shapes=[
            pltpu.VMEM((8, 2, 256, 1792), BF),
            pltpu.VMEM((4, 4, 512, 256), BF),
            pltpu.VMEM((16, 512, 256), BF),
            pltpu.VMEM((16, 512, 512), BF),
            pltpu.VMEM((16, 512, 512), BF),
            pltpu.VMEM((4, 6, 128, 512), BF),
            pltpu.VMEM((4, 6, 128, 512), BF),
            pltpu.VMEM((3, 256, 512), BF),
            pltpu.VMEM((3, 256, 512), BF),
            pltpu.VMEM((3, 256, 512), BF),
            pltpu.VMEM((3, 256, 512), BF),
            pltpu.VMEM((512, 1792), F32),
            pltpu.VMEM((512, 512), F32),
            pltpu.SemaphoreType.DMA((5,)),
            pltpu.SemaphoreType.DMA((16,)),
            pltpu.SemaphoreType.DMA((N1,)),
            pltpu.SemaphoreType.DMA((N1,)),
        ],
        compiler_params=pltpu.CompilerParams(
            collective_id=0, has_side_effects=True, vmem_limit_bytes=67043328
        ),
    )(attn, wout, resid, sin, gain, wg, wu)


N2 = 192


def second_kernel(
    hid, wd_hbm, pj_hbm, xrow, th, tgain, dest,
    out, res, loss,
    w2, pj, tg, pt, so, r1, s1, r2, stat_in, stat_s, loss_in, loss_s, loc, ss, rs,
):
    x, c, z, y = (lax.axis_index(a) for a in AXES)
    t = z * 4 + y
    d = x * 2 + c

    def at(base, k):
        return lax.rem(base + k, 4)

    xr, xl, xo = at(x, 1), at(x, 3), at(x, 2)
    sib = {"c": 1 - c}
    right, left = {"x": xr}, {"x": xl}
    w2_loads, pj_loads = [], []
    for h in range(2):
        w2_loads.append(pltpu.make_async_copy(wd_hbm.at[:, pl.ds(h * 256, 256)], w2.at[d, h], loc.at[h]))
        pj_loads.append(pltpu.make_async_copy(pj_hbm.at[pl.ds(h * 256, 256)], pj.at[d, h], loc.at[2 + h]))
    for cp in w2_loads + pj_loads:
        cp.start()
    greet(
        [sib, right, left]
        + [{"z": at(z, i), "y": at(y, j)} for i in range(4) for j in range(4) if (i, j) != (0, 0)]
    )
    net = Net(ss, rs)
    owner = {"I": x, "L": xl, "R": xr, "O": xo}
    half = {"A": 0, "B": 1}

    def shard(role, core):
        return owner[role[0]] * 2 + core, half[role[1]]

    def along_x_open(tag, buf):
        net.send(tag + "LA", buf.at[d, 0], buf.at[d, 0], right)
        net.send(tag + "RB", buf.at[d, 1], buf.at[d, 1], left)
        net.send(tag + "LB", buf.at[d, 1], buf.at[d, 1], right)
        net.send(tag + "RA", buf.at[d, 0], buf.at[d, 0], left)
        net.send(tag + "sIA", buf.at[d, 0], buf.at[d, 0], sib)
        net.send(tag + "sIB", buf.at[d, 1], buf.at[d, 1], sib)

    def along_x_take(tag, buf, role):
        ref = buf.at[shard(role, c)]
        net.got(tag + role)
        if role == "LA":
            net.send(tag + "OA", ref, ref, right)
        if role == "RB":
            net.send(tag + "OB", ref, ref, left)
        net.send(tag + "s" + role, ref, ref, sib)

    groups = (("IA", "IB"), ("LA", "RB"), ("LB", "RA"), ("OA", "OB"))

    def partial(g, pq):
        core = c if pq == 0 else 1 - c
        for i in range(2):
            term = jnp.dot(hid[...], w2[shard(groups[g][i], core)], preferred_element_type=F32)
            pt[g, pq, :, :, :, i * 256:(i + 1) * 256] = term.astype(BF).reshape(4, 4, 32, 256)
        for j in (1, 2, 3):
            if pq == 0:
                yy = at(y, j)
                net.send(f"a{g}0{j}", pt.at[g, 0, :, yy], r1.at[g, 0, j - 1], {"y": yy})
            else:
                zz = at(z, j)
                net.send(f"a{g}1{j}", pt.at[g, 1, zz], r1.at[g, 1, j - 1], {"z": zz})

    own_sum = {}

    def middle(g, pq):
        net.got(*[f"a{g}{pq}{j}" for j in (1, 2, 3)])
        for k in (1, 2, 3, 0):
            other = at(z if pq == 0 else y, k)
            mine = pt[g, 0, other, y] if pq == 0 else pt[g, 1, z, other]
            s = mine.astype(F32)
            for j in range(3):
                s = s + r1[g, pq, j, other].astype(F32)
            if k == 0:
                own_sum[g, pq] = s
            else:
                s1[g, pq, k - 1] = s.astype(BF)
                dev = {"z": other} if pq == 0 else {"y": other}
                net.send(f"b{g}{pq}{k}", s1.at[g, pq, k - 1], r2.at[g, pq, k - 1], dev)

    def finish(g, pq):
        net.got(*[f"b{g}{pq}{j}" for j in (1, 2, 3)])
        s = own_sum[g, pq]
        for j in range(3):
            s = s + r2[g, pq, j].astype(F32)
        core = c if pq == 0 else 1 - c
        for i in range(2):
            dd, h = shard(groups[g][i], core)
            xin = xrow[dd * 2 + h].astype(F32)
            so[g, pq, z, y, :, i * 256:(i + 1) * 256] = (xin + s[:, i * 256:(i + 1) * 256]).astype(BF)
        ref = so.at[g, pq, z, y]
        for j in (1, 2, 3):
            dev = {"y": at(y, j)} if pq == 0 else {"z": at(z, j)}
            net.send(f"c{g}{pq}{j}", ref, ref, dev)

    def spread_parts(g, pq):
        if pq == 0:
            return "z", z, lambda k, h: so.at[g, 0, at(z, k), pl.ds(2 * h, 2)]
        return "y", y, lambda k, h: so.at[g, 1, pl.ds(2 * h, 2), at(y, k)]

    def spread_open(g, pq):
        net.got(*[f"c{g}{pq}{j}" for j in (1, 2, 3)])
        axis, base, ref = spread_parts(g, pq)
        tag = f"d{g}{pq}"
        up, down = {axis: at(base, 1)}, {axis: at(base, 3)}
        net.send(tag + "LA", ref(0, 0), ref(0, 0), up)
        net.send(tag + "RB", ref(0, 1), ref(0, 1), down)
        net.send(tag + "LB", ref(0, 1), ref(0, 1), up)
        net.send(tag + "RA", ref(0, 0), ref(0, 0), down)

    def spread_forward(g, pq):
        axis, base, ref = spread_parts(g, pq)
        tag = f"d{g}{pq}"
        net.got(tag + "LA")
        net.send(tag + "OA", ref(3, 0), ref(3, 0), {axis: at(base, 1)})
        net.got(tag + "RB")
        net.send(tag + "OB", ref(1, 1), ref(1, 1), {axis: at(base, 3)})

    def spread_close(g, pq):
        tag = f"d{g}{pq}"
        net.got(tag + "LB", tag + "RA", tag + "OA", tag + "OB")

    def predict(g):
        spread_close(g, 0)
        spread_close(g, 1)
        for pq in range(2):
            core = c if pq == 0 else 1 - c
            left_side = so[g, pq].reshape(512, 512)
            total = None
            for i in range(2):
                term = jnp.dot(
                    left_side[:, i * 256:(i + 1) * 256],
                    pj[shard(groups[g][i], core)],
                    preferred_element_type=F32,
                )
                total = term if total is None else total + term
            if g == 0 and pq == 0:
                res[...] = total
            else:
                res[...] += total

    def row_squares(value):
        v = value * value
        v = v[:, 0:128] + v[:, 128:256] + v[:, 256:384] + v[:, 384:512]
        v = v.T
        parts = v[0:8, :]
        for i in range(1, 16):
            parts = parts + v[8 * i:8 * i + 8, :]
        return parts

    others = [(i, j) for i in range(4) for j in range(4) if (i, j) != (0, 0)]

    def stat_open(tag, own, inbox):
        for n, (i, j) in enumerate(others):
            net.send(f"{tag}{n}", own, inbox.at[n], {"z": at(z, i), "y": at(y, j)})

    def stat_take(tag, own, inbox):
        net.got(*[f"{tag}{n}" for n in range(15)])
        total = own[...]
        for n in range(15):
            total = total + inbox[n]
        return jnp.sum(total, axis=0, keepdims=True)

    def landed(g):
        return target_of(groups[g], c) + target_of(groups[g], 1 - c)

    def target_of(roles, core):
        return [shard(r, core) for r in roles]

    row_id = d * 512 + lax.broadcasted_iota(jnp.int32, (512, 256), 0)

    def subtract_target(slots):
        total = None
        for dd, h in slots:
            pick = dest[dd * 2 + h]
            onehot = jnp.where(row_id == pick, 1.0, 0.0).astype(BF)
            term = jnp.dot(onehot, tg[dd, h], preferred_element_type=F32)
            total = term if total is None else total + term
        res[...] -= total

    def finish_target():
        scale = lax.rsqrt(stat_take("q", stat_s, stat_in) / HT + 1e-06)
        scale = jnp.broadcast_to(scale, (128, 512)).T
        gain = tgain[t].astype(F32)
        for h in range(2):
            for i in range(4):
                rows, cols = slice(h * 256, h * 256 + 256), slice(i * 128, i * 128 + 128)
                tg[d, h, :, cols] = (th[rows, cols] * scale[rows, :] * gain[:, cols]).astype(BF)

    def both(step, g):
        step(g, 0)
        step(g, 1)

    def take_two(tag, buf, g):
        along_x_take(tag, buf, groups[g][0])
        along_x_take(tag, buf, groups[g][1])

    def sibling_has(tag, g):
        net.got(tag + "s" + groups[g][0], tag + "s" + groups[g][1])

    def partials(g):
        partial(g, 0)
        sibling_has("w", g)
        partial(g, 1)

    for cp in w2_loads:
        cp.wait()
    along_x_open("w", w2)
    partial(0, 0)
    stat_s[...] = row_squares(th[...])
    stat_open("q", stat_s, stat_in)
    sibling_has("w", 0)
    partial(0, 1)
    both(middle, 0)
    finish_target()
    take_two("w", w2, 1)
    partials(1)
    for cp in pj_loads:
        cp.wait()
    along_x_open("p", pj)
    both(finish, 0)
    both(spread_open, 0)
    both(middle, 1)
    take_two("w", w2, 2)
    partials(2)
    both(spread_forward, 0)
    both(finish, 1)
    both(spread_open, 1)
    both(middle, 2)
    take_two("w", w2, 3)
    partials(3)
    both(spread_forward, 1)
    both(finish, 2)
    take_two("p", pj, 1)
    along_x_open("t", tg)
    both(spread_open, 2)
    both(middle, 3)
    sibling_has("p", 0)
    predict(0)
    both(spread_forward, 2)
    both(finish, 3)
    take_two("p", pj, 2)
    sibling_has("p", 1)
    predict(1)
    both(spread_open, 3)
    take_two("p", pj, 3)
    sibling_has("p", 2)
    predict(2)
    both(spread_forward, 3)
    take_two("t", tg, 1)
    sibling_has("t", 0)
    subtract_target(landed(0))
    sibling_has("p", 3)
    predict(3)
    take_two("t", tg, 2)

    h0 = lax.rem(t, 2)
    d0 = lax.div(t, 2)
    k0 = lax.rem(lax.div(d0, 2) - x + 4, 4)
    k_odd, k_two = lax.rem(k0, 2), lax.div(k0, 2)
    g0 = (1 - k_odd) * k_two * 3 + k_odd * (k_two * (1 + h0) + (1 - k_two) * (2 - h0))
    i0 = (1 - k_odd) * h0 + k_odd * (1 - k_two)
    pq0 = lax.rem(d0 + c, 2)
    out[...] = so[g0, pq0, :, :, :, pl.ds(pl.multiple_of(i0 * 256, 256), 256)].reshape(512, 256)

    sibling_has("t", 1)
    subtract_target(landed(1))
    sibling_has("t", 2)
    subtract_target(landed(2))
    take_two("t", tg, 3)
    sibling_has("t", 3)
    subtract_target(landed(3))

    loss_s[...] = row_squares(res[...])
    stat_open("l", loss_s, loss_in)
    loss[...] = stat_take("l", loss_s, loss_in) / HT
    net.drain()


def call_second(hid, wd, pj, xrow, th, tgain, dest):
    vm = pl.BlockSpec(memory_space=pltpu.VMEM)
    hb = pl.BlockSpec(memory_space=pl.ANY)
    return pl.pallas_call(
        second_kernel,
        name="second",
        out_shape=(
            jax.ShapeDtypeStruct((512, 256), BF),
            jax.ShapeDtypeStruct((512, 512), F32),
            jax.ShapeDtypeStruct((1, 512), F32),
        ),
        in_specs=[vm, hb, hb, vm, vm, vm, vm],
        out_specs=(vm, vm, vm),
        scratch_shapes=[
            pltpu.VMEM((8, 2, 896, 256), BF),
            pltpu.VMEM((8, 2, 256, 512), BF),
            pltpu.VMEM((8, 2, 256, 512), BF),
            pltpu.VMEM((4, 2, 4, 4, 32, 512), BF),
            pltpu.VMEM((4, 2, 4, 4, 32, 512), BF),
            pltpu.VMEM((4, 2, 3, 4, 32, 512), BF),
            pltpu.VMEM((4, 2, 3, 32, 512), BF),
            pltpu.VMEM((4, 2, 3, 32, 512), BF),
            pltpu.VMEM((15, 8, 512), F32),
            pltpu.VMEM((8, 512), F32),
            pltpu.VMEM((15, 8, 512), F32),
            pltpu.VMEM((8, 512), F32),
            pltpu.SemaphoreType.DMA((4,)),
            pltpu.SemaphoreType.DMA((N2,)),
            pltpu.SemaphoreType.DMA((N2,)),
        ],
        compiler_params=pltpu.CompilerParams(
            collective_id=1, has_side_effects=True, vmem_limit_bytes=67043328
        ),
    )(hid, wd, pj, xrow, th, tgain, dest)


def local(
    attn_ctx,
    w_out,
    resid,
    teacher_gain,
    dest_row,
    student_in,
    student_gain,
    w_gate,
    w_up,
    w_down,
    proj,
):
    hidden, th, xrow = call_first(
        attn_ctx, w_out, resid, student_in, student_gain.reshape(16, 256), w_gate, w_up
    )
    out, residue, loss = call_second(
        hidden, w_down, proj, xrow, th, teacher_gain.reshape(16, 1, 512), dest_row.reshape(16, 1, 256)
    )
    return (out, loss.reshape(512), residue)


def solution(mesh):
    torus = Mesh(mesh.devices.reshape(4, 2, 4, 4), AXES)
    in_specs = (
        P(DP, TENSOR),
        P(TENSOR, None),
        P(DP + TENSOR, None),
        P(),
        P(),
        P(DP, TENSOR),
        P(),
        P(DP, TENSOR),
        P(DP, TENSOR),
        P(TENSOR, DP),
        P(DP, TENSOR),
    )
    out_specs = (P(DP, TENSOR), P(DP), P(DP, TENSOR))
    return jax.shard_map(local, mesh=torus, in_specs=in_specs, out_specs=out_specs, check_vma=False)
```

```python
import jax
import jax.numpy as jnp
from jax import lax
from jax.sharding import Mesh
from jax.sharding import PartitionSpec as P
from jax.experimental import pallas as pl
from jax.experimental.pallas import tpu as pltpu

HT = 8192
BF = jnp.bfloat16
F32 = jnp.float32
AXES = ("x", "c", "z", "y")
TENSOR = ("z", "y")
DP = ("x", "c")
TRANSFERS = 284


class Net:
    def __init__(self, send_sems, recv_sems):
        self.ss, self.rs, self.made, self.left = send_sems, recv_sems, {}, set()

    def send(self, role, src, dst, dev):
        i = len(self.made)
        cp = pltpu.make_async_remote_copy(
            src_ref=src,
            dst_ref=dst,
            send_sem=self.ss.at[i],
            recv_sem=self.rs.at[i],
            device_id=dev,
            device_id_type=pl.DeviceIdType.MESH,
        )
        cp.start()
        self.made[role] = cp
        self.left.add(role)

    def got(self, *roles):
        for role in roles:
            self.made[role].wait_recv()

    def flush(self, *roles):
        for role in roles:
            self.made[role].wait_send()
            self.left.remove(role)

    def drain(self):
        self.flush(*[role for role in self.made if role in self.left])


def greet(partners):
    barrier = pltpu.get_barrier_semaphore()
    for dev in partners:
        pl.semaphore_signal(barrier, inc=1, device_id=dev, device_id_type=pl.DeviceIdType.MESH)
    pl.semaphore_wait(barrier, len(partners))


def kernel(
    attn, wout_hbm, resid, sin, gain, wg_hbm, wu_hbm, wd_hbm, pj_hbm, tgain, dest,
    out, res, loss,
    w1, xg, wout, part, rp, rq, sp, sq, rp2, rq2, acc, hid, xrow, w2, pj, r1, r2,
    stat_in, stat_s, loss_in, loss_s, loc, wsem, plane, ss, rs,
):
    x, c, z, y = (lax.axis_index(a) for a in AXES)
    t = z * 4 + y
    d = x * 2 + c

    def at(base, k):
        return lax.rem(base + k, 4)

    xr, xl, xo = at(x, 1), at(x, 3), at(x, 2)
    sib = {"c": 1 - c}
    right, left = {"x": xr}, {"x": xl}
    loads, w2_loads, pj_loads = [], [], []
    for h in range(2):
        rows = pl.ds(h * 256, 256)
        loads.append(pltpu.make_async_copy(wg_hbm.at[rows], w1.at[d, h, :, pl.ds(0, 896)], loc.at[2 * h]))
        loads.append(pltpu.make_async_copy(wu_hbm.at[rows], w1.at[d, h, :, pl.ds(896, 896)], loc.at[2 * h + 1]))
        w2_loads.append(pltpu.make_async_copy(wd_hbm.at[:, rows], w2.at[d, h], loc.at[5 + h]))
        pj_loads.append(pltpu.make_async_copy(pj_hbm.at[rows], pj.at[d, h], loc.at[7 + h]))
    loads.append(pltpu.make_async_copy(sin, xg.at[z, y], loc.at[4]))
    for cp in loads:
        cp.start()

    order = (
        (1, 1), (1, 2), (2, 1), (1, 3), (3, 1), (2, 2), (2, 3), (3, 2), (3, 3),
        (0, 1), (1, 0), (0, 2), (2, 0), (0, 3), (3, 0), (0, 0),
    )
    SLOTS = 4

    def block_cols(dz, dy):
        return pl.ds(pl.multiple_of((at(z, dz) * 4 + at(y, dy)) * 512, 512), 512)

    wloads = [
        pltpu.make_async_copy(wout_hbm.at[:, block_cols(*b)], wout.at[i % SLOTS], wsem.at[i % SLOTS])
        for i, b in enumerate(order)
    ]

    others = [(i, j) for i in range(4) for j in range(4) if (i, j) != (0, 0)]
    greet([sib, right, left] + [{a: at(b, k)} for a, b in (("y", y), ("z", z)) for k in (1, 2, 3)])
    net = Net(ss, rs)
    for k in (1, 2, 3):
        pl.semaphore_signal(plane, inc=1, device_id={"y": at(y, k)}, device_id_type=pl.DeviceIdType.MESH)

    def ring_open(tag, axis, base, ref, src=None):
        up, down = {axis: at(base, 1)}, {axis: at(base, 3)}
        src = src or (lambda h: ref(0, h))
        net.send(tag + "LA", src(0), ref(0, 0), up)
        net.send(tag + "RB", src(1), ref(0, 1), down)
        net.send(tag + "LB", src(1), ref(0, 1), up)
        net.send(tag + "RA", src(0), ref(0, 0), down)

    def ring_forward(tag, axis, base, ref):
        net.got(tag + "LA")
        net.send(tag + "OA", ref(3, 0), ref(3, 0), {axis: at(base, 1)})
        net.got(tag + "RB")
        net.send(tag + "OB", ref(1, 1), ref(1, 1), {axis: at(base, 3)})

    RING = ("LA", "RB", "LB", "RA", "OA", "OB")

    def ring_close(tag):
        net.got(*[tag + role for role in RING[2:]])

    p1 = lambda k, h: xg.at[z, at(y, k), h]
    q1 = lambda k, h: xg.at[at(z, k), y, 2 + h]
    p2 = lambda k, h: xg.at[at(z, k), :, h]
    q2 = lambda k, h: xg.at[:, at(y, k), 2 + h]

    owner = {"I": x, "L": xl, "R": xr, "O": xo}
    half = {"A": 0, "B": 1}
    groups = (("IA", "IB"), ("LA", "RB"), ("LB", "RA"), ("OA", "OB"))

    def shard(role, core):
        return owner[role[0]] * 2 + core, half[role[1]]

    w1_ref = lambda role, core: w1.at[shard(role, core)]
    w2_ref = lambda role, core: w2.at[shard(role, core)]
    pj_ref = lambda role, core: pj.at[shard(role, core)]

    def tg_ref(role, core):
        dd, h = shard(role, core)
        return w1.at[dd, h, :, pl.ds(0, 512)]

    def along_x_open(tag, ref):
        for role, own, dev in (("LA", "IA", right), ("RB", "IB", left), ("LB", "IB", right), ("RA", "IA", left)):
            net.send(tag + role, ref(own, c), ref(own, c), dev)
        for own in groups[0]:
            net.send(tag + "s" + own, ref(own, c), ref(own, c), sib)

    def along_x_take(tag, ref, g):
        for role in groups[g]:
            net.got(tag + role)
            block = ref(role, c)
            if role == "LA":
                net.send(tag + "OA", block, block, right)
            if role == "RB":
                net.send(tag + "OB", block, block, left)
            net.send(tag + "s" + role, block, block, sib)

    def sibling_has(tag, g):
        net.got(*[tag + "s" + role for role in groups[g]])

    def partial(i):
        b = order[i]
        wloads[i].wait()
        acc[:, :512] = jnp.dot(attn[...], wout[i % SLOTS], preferred_element_type=F32)
        if i + SLOTS < 16:
            wloads[i + SLOTS].start()
        rows = pl.ds(pl.multiple_of(t * 32, 32), 32)
        acc[rows, :512] += resid[:, block_cols(*b)].astype(F32)
        part[b[0] * 4 + b[1]] = acc[:, :512].astype(BF).reshape(4, 4, 32, 512)

    inbox = (rp, rq)

    def term(pq, k, j, h):
        return (k * 4 + j if pq == 0 else j * 4 + k), pq * 2 + h

    def sum_send(name, pq, k, j, h, slot, to):
        dev = {"y": at(y, to)} if pq == 0 else {"z": at(z, to)}
        net.send(f"{name}{pq}{k}", part.at[term(pq, k, j, h)], inbox[pq].at[k, slot], dev)

    def sum_open(k):
        for pq in range(2):
            sum_send("fA", pq, k, 2, 0, 0, 1)
            sum_send("fB", pq, k, 2, 1, 1, 3)
            sum_send("uB", pq, k, 1, 1, 3, 1)
            sum_send("dA", pq, k, 3, 0, 4, 3)

    def sum_pass(k):
        for pq in range(2):
            for name, j, h, slot, to_slot, send_as, to in (("fA", 1, 0, 0, 2, "uA", 1), ("fB", 3, 1, 1, 5, "dB", 3)):
                net.got(f"{name}{pq}{k}")
                b, rows = term(pq, k, j, h)
                part[b, rows] = (part[b, rows].astype(F32) + inbox[pq][k, slot].astype(F32)).astype(BF)
                sum_send(send_as, pq, k, j, h, to_slot, to)

    SUMS = ("fA", "fB", "uB", "dA", "uA", "dB")

    def sum_close(k):
        for pq in range(2):
            net.got(*[f"{name}{pq}{k}" for name in ("uA", "uB", "dA", "dB")])
            store, box = (sp, rp2) if pq == 0 else (sq, rq2)
            for h in range(2):
                b, rows = term(pq, k, 0, h)
                s = part[b, rows].astype(F32)
                s = s + inbox[pq][k, 2 + h].astype(F32) + inbox[pq][k, 4 + h].astype(F32)
                if k == 0:
                    res[pq * 256 + h * 128:pq * 256 + h * 128 + 128, :] = s.reshape(128, 512)
                else:
                    store[k - 1, h] = s.astype(BF)
            if k:
                dev = {"z": at(z, k)} if pq == 0 else {"y": at(y, k)}
                net.send(f"v{pq}{k}", store.at[k - 1], box.at[k - 1], dev)

    def teacher_hidden():
        for k in (1, 2, 3):
            net.got(f"v0{k}", f"v1{k}")
        for pq, box in ((0, rp2), (1, rq2)):
            rows = slice(pq * 256, pq * 256 + 256)
            s = box[0].astype(F32) + box[1].astype(F32) + box[2].astype(F32)
            res[rows, :] += s.reshape(256, 512)

    def slot_of(role, core):
        return xg.at[owner[role[0]], 2 * core + half[role[1]]]

    def gate_up(g):
        @pl.loop(0, 7)
        def _(j):
            cols = pl.ds(pl.multiple_of(j * 256, 256), 256)
            total = None
            for core in (c, 1 - c):
                for role in groups[g]:
                    dd, h = shard(role, core)
                    lhs = slot_of(role, core)[...].reshape(512, 256)
                    term = jnp.dot(lhs, w1[dd, h, :, cols], preferred_element_type=F32)
                    total = term if total is None else total + term
            if g == 0:
                acc[:, cols] = total
            else:
                acc[:, cols] += total

    free_blocks = ((5, 6), (7, 9), (10, 11), (13, 14))

    def down(g, pq):
        core = c if pq == 0 else 1 - c
        b = free_blocks[g][pq]
        for i in range(2):
            dd, h = shard(groups[g][i], core)
            piece = jnp.dot(hid[...], w2[dd, h], preferred_element_type=F32)
            part[b, :, :, :, i * 256:(i + 1) * 256] = piece.astype(BF).reshape(4, 4, 32, 256)
        for j in (1, 2, 3):
            if pq == 0:
                yy = at(y, j)
                net.send(f"a{g}0{j}", part.at[b, :, yy], r1.at[g, 0, j - 1], {"y": yy})
            else:
                zz = at(z, j)
                net.send(f"a{g}1{j}", part.at[b, zz], r1.at[g, 1, j - 1], {"z": zz})

    own_sum = {}

    def middle(g, pq):
        net.got(*[f"a{g}{pq}{j}" for j in (1, 2, 3)])
        b = free_blocks[g][pq]
        for k in (1, 2, 3, 0):
            other = at(z if pq == 0 else y, k)
            mine = part[b, other, y] if pq == 0 else part[b, z, other]
            s = mine.astype(F32)
            for j in range(3):
                s = s + r1[g, pq, j, other].astype(F32)
            if k == 0:
                own_sum[g, pq] = s
            else:
                n = (2 * g + pq) * 3 + k - 1
                where = (n // 8, n // 4 % 2, n % 4)
                sp[where] = s.astype(BF)
                dev = {"z": other} if pq == 0 else {"y": other}
                net.send(f"b{g}{pq}{k}", sp.at[where], r2.at[g, pq, k - 1], dev)

    def finish(g, pq):
        net.got(*[f"b{g}{pq}{j}" for j in (1, 2, 3)])
        s = own_sum[g, pq]
        for j in range(3):
            s = s + r2[g, pq, j].astype(F32)
        core = c if pq == 0 else 1 - c
        for i in range(2):
            dd, h = shard(groups[g][i], core)
            xin = xrow[dd * 2 + h].astype(F32)
            xg[g, 2 * pq + i, z, y] = (xin + s[:, i * 256:(i + 1) * 256]).astype(BF)
        ref = xg.at[g, pl.ds(2 * pq, 2), z, y]
        for j in (1, 2, 3):
            dev = {"y": at(y, j)} if pq == 0 else {"z": at(z, j)}
            net.send(f"c{g}{pq}{j}", ref, ref, dev)

    def spread_ring(g, pq):
        pair = pl.ds(2 * pq, 2)
        if pq == 0:
            return f"d{g}0", "z", z, lambda k, h: xg.at[g, pair, at(z, k), pl.ds(2 * h, 2)]
        return f"d{g}1", "y", y, lambda k, h: xg.at[g, pair, pl.ds(2 * h, 2), at(y, k)]

    def spread_open(g, pq):
        net.got(*[f"c{g}{pq}{j}" for j in (1, 2, 3)])
        ring_open(*spread_ring(g, pq))

    def spread_forward(g, pq):
        ring_forward(*spread_ring(g, pq))

    def predict(g):
        ring_close(f"d{g}0")
        ring_close(f"d{g}1")
        total = None
        for pq in range(2):
            core = c if pq == 0 else 1 - c
            for i in range(2):
                dd, h = shard(groups[g][i], core)
                lhs = xg[g, 2 * pq + i].reshape(512, 256)
                piece = jnp.dot(lhs, pj[dd, h], preferred_element_type=F32)
                total = piece if total is None else total + piece
        if g == 0:
            res[...] = total
        else:
            res[...] += total

    def row_squares(value):
        v = value * value
        v = v[:, 0:128] + v[:, 128:256] + v[:, 256:384] + v[:, 384:512]
        v = v.T
        parts = v[0:8, :]
        for i in range(1, 16):
            parts = parts + v[8 * i:8 * i + 8, :]
        return parts

    def stat_open(tag, own, box):
        for n, (i, j) in enumerate(others):
            net.send(f"{tag}{n}", own, box.at[n], {"z": at(z, i), "y": at(y, j)})

    def stat_take(tag, own, box):
        net.got(*[f"{tag}{n}" for n in range(15)])
        total = own[...]
        for n in range(15):
            total = total + box[n]
        return jnp.sum(total, axis=0, keepdims=True)

    def finish_target():
        scale = lax.rsqrt(stat_take("q", stat_s, stat_in) / HT + 1e-06)
        scale = jnp.broadcast_to(scale, (128, 512)).T
        eight = tgain[pl.ds(pl.multiple_of(lax.div(t, 2) * 8, 8), 8), :].astype(F32)
        four = jnp.where(lax.rem(t, 2) == 0, eight[0:4, :], eight[4:8, :])
        for h in range(2):
            for i in range(4):
                rows, cols = slice(h * 256, h * 256 + 256), slice(i * 128, i * 128 + 128)
                w1[d, h, :, cols] = (res[rows, cols] * scale[rows, :] * four[i:i + 1, :]).astype(BF)

    row_id = d * 512 + lax.broadcasted_iota(jnp.int32, (512, 256), 0)

    def subtract_target(g):
        total = None
        for core in (c, 1 - c):
            for role in groups[g]:
                dd, h = shard(role, core)
                onehot = jnp.where(row_id == dest[dd * 2 + h], 1.0, 0.0).astype(BF)
                piece = jnp.dot(onehot, w1[dd, h, :, 0:512], preferred_element_type=F32)
                total = piece if total is None else total + piece
        res[...] -= total

    def both(step, g):
        step(g, 0)
        step(g, 1)

    def downs(g):
        down(g, 0)
        sibling_has("m", g)
        down(g, 1)

    ring_open("p1", "y", y, p1, lambda h: sin.at[h])
    ring_open("q1", "z", z, q1, lambda h: sin.at[2 + h])
    for cp in loads[:4]:
        cp.wait()
    along_x_open("w", w1_ref)
    for i in range(SLOTS):
        wloads[i].start()
    for cp in w2_loads + pj_loads:
        cp.start()
    for i in range(5):
        partial(i)
    ring_forward("p1", "y", y, p1)
    ring_forward("q1", "z", z, q1)
    sum_open(1)
    partial(5)
    partial(6)
    loads[4].wait()
    ring_close("p1")
    ring_open("p2", "z", z, p2)
    ring_close("q1")
    ring_open("q2", "y", y, q2)
    partial(7)
    partial(8)
    sum_pass(1)
    for i in range(9, 16):
        partial(i)
    sum_open(2)
    ring_forward("p2", "z", z, p2)
    ring_forward("q2", "y", y, q2)
    sum_open(3)
    along_x_take("w", w1_ref, 1)
    for cp in w2_loads:
        cp.wait()
    along_x_open("m", w2_ref)
    sum_pass(2)
    sum_open(0)
    ring_close("p2")
    ring_close("q2")
    for tag in ("p1", "q1", "p2", "q2"):
        net.flush(*[tag + role for role in RING])
    xrow[...] = xg[:, :, z, y].reshape(16, 32, 256)

    @pl.loop(0, 4)
    def _(r):
        total = jnp.zeros((128, 256), F32)
        for s in range(16):
            v = xg[s // 4, s % 4, r].reshape(128, 256).astype(F32)
            total = total + v * v
        scale = lax.rsqrt(jnp.sum(total, axis=1, keepdims=True) / 4096.0 + 1e-05)
        for s in range(16):
            v = xg[s // 4, s % 4, r].reshape(128, 256).astype(F32)
            g = jnp.concatenate([gain[2 * s:2 * s + 1, :], gain[2 * s + 1:2 * s + 2, :]], axis=1)
            xg[s // 4, s % 4, r] = (v * scale * g.astype(F32)).astype(BF).reshape(4, 32, 256)

    sum_pass(3)
    sibling_has("w", 0)
    gate_up(0)
    sum_close(1)
    sibling_has("w", 1)
    gate_up(1)
    along_x_take("w", w1_ref, 2)
    sum_pass(0)
    sum_close(2)
    sibling_has("w", 2)
    gate_up(2)
    sum_close(3)
    along_x_take("w", w1_ref, 3)
    sibling_has("w", 3)
    gate_up(3)

    @pl.loop(0, 7)
    def _(j):
        g = acc[:, pl.ds(pl.multiple_of(j * 128, 128), 128)]
        u = acc[:, pl.ds(pl.multiple_of(896 + j * 128, 128), 128)]
        hid[:, pl.ds(pl.multiple_of(j * 128, 128), 128)] = (jax.nn.silu(g) * u).astype(BF)

    net.flush(*[f"{name}{pq}{k}" for name in SUMS for pq in range(2) for k in (1, 2, 3)])
    net.flush(*[f"v0{k}" for k in (1, 2, 3)])
    downs(0)
    net.flush(*["w" + s + role for g in groups for role in g for s in ("", "s") if s or role[0] != "I"])
    for cp in pj_loads:
        cp.wait()
    sum_close(0)
    along_x_take("m", w2_ref, 1)
    along_x_open("p", pj_ref)
    downs(1)
    both(middle, 0)
    teacher_hidden()
    stat_s[...] = row_squares(res[...])
    pl.semaphore_wait(plane, 3)
    stat_open("q", stat_s, stat_in)
    both(middle, 1)
    both(finish, 0)
    along_x_take("m", w2_ref, 2)
    downs(2)
    both(finish, 1)
    both(spread_open, 0)
    finish_target()
    both(middle, 2)
    along_x_take("m", w2_ref, 3)
    downs(3)
    both(spread_open, 1)
    both(spread_forward, 0)
    both(finish, 2)
    along_x_take("p", pj_ref, 1)
    sibling_has("p", 0)
    along_x_open("t", tg_ref)
    both(middle, 3)
    along_x_take("p", pj_ref, 2)
    both(spread_forward, 1)
    both(spread_open, 2)
    predict(0)
    both(finish, 3)
    along_x_take("p", pj_ref, 3)
    both(spread_forward, 2)
    sibling_has("p", 1)
    predict(1)
    both(spread_open, 3)
    along_x_take("t", tg_ref, 1)
    both(spread_forward, 3)
    sibling_has("p", 2)
    predict(2)
    sibling_has("t", 0)
    subtract_target(0)
    along_x_take("t", tg_ref, 2)
    sibling_has("p", 3)
    predict(3)

    h0 = lax.rem(t, 2)
    d0 = lax.div(t, 2)
    k0 = lax.rem(lax.div(d0, 2) - x + 4, 4)
    k_odd, k_two = lax.rem(k0, 2), lax.div(k0, 2)
    g0 = (1 - k_odd) * k_two * 3 + k_odd * (k_two * (1 + h0) + (1 - k_two) * (2 - h0))
    i0 = (1 - k_odd) * h0 + k_odd * (1 - k_two)
    out[...] = xg[g0, 2 * lax.rem(d0 + c, 2) + i0].reshape(512, 256)

    sibling_has("t", 1)
    subtract_target(1)
    sibling_has("t", 2)
    subtract_target(2)
    along_x_take("t", tg_ref, 3)
    sibling_has("t", 3)
    subtract_target(3)
    loss_s[...] = row_squares(res[...])
    stat_open("l", loss_s, loss_in)
    loss[...] = stat_take("l", loss_s, loss_in) / HT
    net.drain()


def call_kernel(*args):
    vm = pl.BlockSpec(memory_space=pltpu.VMEM)
    hb = pl.BlockSpec(memory_space=pl.ANY)
    return pl.pallas_call(
        kernel,
        name="first",
        out_shape=(
            jax.ShapeDtypeStruct((512, 256), BF),
            jax.ShapeDtypeStruct((512, 512), F32),
            jax.ShapeDtypeStruct((1, 512), F32),
        ),
        in_specs=[vm, hb, vm, vm, vm, hb, hb, hb, hb, vm, vm],
        out_specs=(vm, vm, vm),
        scratch_shapes=[
            pltpu.VMEM((8, 2, 256, 1792), BF),
            pltpu.VMEM((4, 4, 4, 4, 32, 256), BF),
            pltpu.VMEM((4, 512, 512), BF),
            pltpu.VMEM((16, 4, 4, 32, 512), BF),
            pltpu.VMEM((4, 6, 4, 32, 512), BF),
            pltpu.VMEM((4, 6, 4, 32, 512), BF),
            pltpu.VMEM((3, 2, 4, 32, 512), BF),
            pltpu.VMEM((3, 2, 4, 32, 512), BF),
            pltpu.VMEM((3, 2, 4, 32, 512), BF),
            pltpu.VMEM((3, 2, 4, 32, 512), BF),
            pltpu.VMEM((512, 1792), F32),
            pltpu.VMEM((512, 896), BF),
            pltpu.VMEM((16, 32, 256), BF),
            pltpu.VMEM((8, 2, 896, 256), BF),
            pltpu.VMEM((8, 2, 256, 512), BF),
            pltpu.VMEM((4, 2, 3, 4, 32, 512), BF),
            pltpu.VMEM((4, 2, 3, 32, 512), BF),
            pltpu.VMEM((15, 8, 512), F32),
            pltpu.VMEM((8, 512), F32),
            pltpu.VMEM((15, 8, 512), F32),
            pltpu.VMEM((8, 512), F32),
            pltpu.SemaphoreType.DMA((9,)),
            pltpu.SemaphoreType.DMA((4,)),
            pltpu.SemaphoreType.REGULAR,
            pltpu.SemaphoreType.DMA((TRANSFERS,)),
            pltpu.SemaphoreType.DMA((TRANSFERS,)),
        ],
        compiler_params=pltpu.CompilerParams(
            collective_id=0, has_side_effects=True, vmem_limit_bytes=67043328
        ),
    )(*args)


def keep(out, res, loss, out_to, res_to, loss_to):
    out_to[...] = out[...]
    res_to[...] = res[...]
    loss_to[...] = loss[...]


def local(
    attn_ctx,
    w_out,
    resid,
    teacher_gain,
    dest_row,
    student_in,
    student_gain,
    w_gate,
    w_up,
    w_down,
    proj,
):
    made = call_kernel(
        attn_ctx,
        w_out,
        resid,
        student_in.reshape(4, 4, 32, 256),
        student_gain.reshape(32, 128),
        w_gate,
        w_up,
        w_down,
        proj,
        teacher_gain.reshape(64, 128),
        dest_row.reshape(16, 1, 256),
    )
    vm = pl.BlockSpec(memory_space=pltpu.VMEM)
    out, residue, loss = pl.pallas_call(
        keep,
        name="keep",
        out_shape=tuple(jax.ShapeDtypeStruct(a.shape, a.dtype) for a in made),
        in_specs=[vm, vm, vm],
        out_specs=(vm, vm, vm),
    )(*made)
    return (out, loss.reshape(512), residue)


def solution(mesh):
    torus = Mesh(mesh.devices.reshape(4, 2, 4, 4), AXES)
    in_specs = (
        P(DP, TENSOR),
        P(TENSOR, None),
        P(DP + TENSOR, None),
        P(),
        P(),
        P(DP, TENSOR),
        P(),
        P(DP, TENSOR),
        P(DP, TENSOR),
        P(TENSOR, DP),
        P(DP, TENSOR),
    )
    out_specs = (P(DP, TENSOR), P(DP), P(DP, TENSOR))
    return jax.shard_map(local, mesh=torus, in_specs=in_specs, out_specs=out_specs, check_vma=False)
```

```python
import jax
import jax.numpy as jnp
from jax import lax
from jax.sharding import Mesh
from jax.sharding import PartitionSpec as P
from jax.experimental import pallas as pl
from jax.experimental.pallas import tpu as pltpu

HT = 8192
BF = jnp.bfloat16
F32 = jnp.float32
AXES = ("x", "c", "z", "y")
TENSOR = ("z", "y")
DP = ("x", "c")
SENDS, RECEIVES = 16, 113


class Net:
    def __init__(self, send_sems, recv_sems):
        self.ss, self.rs, self.sent, self.due, self.made = send_sems, recv_sems, {}, {}, {}

    def send(self, out, role, src, dst, dev):
        i = self.sent.setdefault(out, len(self.sent))
        j = self.due.setdefault(role, len(self.due))
        cp = pltpu.make_async_remote_copy(
            src_ref=src,
            dst_ref=dst,
            send_sem=self.ss.at[i],
            recv_sem=self.rs.at[j],
            device_id=dev,
            device_id_type=pl.DeviceIdType.MESH,
        )
        cp.start()
        self.made[role] = cp

    def got(self, role, bytes_of=None):
        if bytes_of is None:
            self.made[role].wait_recv()
        else:
            pltpu.make_async_copy(bytes_of, bytes_of, self.rs.at[self.due[role]]).wait()

    def flush(self, out, bytes_of):
        pltpu.make_async_copy(bytes_of, bytes_of, self.ss.at[self.sent[out]]).wait()


def greet(partners):
    barrier = pltpu.get_barrier_semaphore()
    for dev in partners:
        pl.semaphore_signal(barrier, inc=1, device_id=dev, device_id_type=pl.DeviceIdType.MESH)
    pl.semaphore_wait(barrier, len(partners))


def kernel(
    attn, wout_hbm, resid, sin, gain, wg_hbm, wu_hbm, wd_hbm, pj_hbm, tgain, dest,
    out, res, loss,
    w1, xg, wout, part, rp, rq, sp, sq, rp2, rq2, acc, hid, xrow, w2, pj, r1, r2,
    stat_in, stat_s, loss_in, loss_s, ranks, ta, loc, wsem, plane, ss, rs,
):
    x, c, z, y = (lax.axis_index(a) for a in AXES)
    t = z * 4 + y
    d = x * 2 + c

    def at(base, k):
        return lax.rem(base + k, 4)

    xr, xl, xo = at(x, 1), at(x, 3), at(x, 2)
    sib = {"c": 1 - c}
    right, left = {"x": xr}, {"x": xl}
    loads, w2_loads, pj_loads = [], [], []
    for h in range(2):
        rows = pl.ds(h * 256, 256)
        loads.append(pltpu.make_async_copy(wg_hbm.at[rows], w1.at[d, h, :, pl.ds(0, 896)], loc.at[2 * h]))
        loads.append(pltpu.make_async_copy(wu_hbm.at[rows], w1.at[d, h, :, pl.ds(896, 896)], loc.at[2 * h + 1]))
        w2_loads.append(pltpu.make_async_copy(wd_hbm.at[:, rows], w2.at[d, h], loc.at[5 + h]))
        pj_loads.append(pltpu.make_async_copy(pj_hbm.at[rows], pj.at[d, h], loc.at[7 + h]))
    loads.append(pltpu.make_async_copy(sin, xg.at[z, y], loc.at[4]))
    for cp in loads:
        cp.start()

    order = (
        (1, 1), (1, 2), (2, 1), (1, 3), (3, 1), (2, 2), (2, 3), (3, 2), (3, 3),
        (0, 1), (1, 0), (0, 2), (2, 0), (0, 3), (3, 0), (0, 0),
    )
    SLOTS = 4

    def block_cols(dz, dy):
        return pl.ds(pl.multiple_of((at(z, dz) * 4 + at(y, dy)) * 512, 512), 512)

    wloads = [
        pltpu.make_async_copy(wout_hbm.at[:, block_cols(*b)], wout.at[i % SLOTS], wsem.at[i % SLOTS])
        for i, b in enumerate(order)
    ]

    others = [(i, j) for i in range(4) for j in range(4) if (i, j) != (0, 0)]
    greet([sib, right, left] + [{a: at(b, k)} for a, b in (("y", y), ("z", z)) for k in (1, 2, 3)])
    net = Net(ss, rs)
    for k in (1, 2, 3):
        pl.semaphore_signal(plane, inc=1, device_id={"y": at(y, k)}, device_id_type=pl.DeviceIdType.MESH)

    def ring_open(out, tag, axis, base, ref, src=None):
        up, down = {axis: at(base, 1)}, {axis: at(base, 3)}
        src = src or (lambda h: ref(0, h))
        net.send(out, tag + "LA", src(0), ref(0, 0), up)
        net.send(out, tag + "RB", src(1), ref(0, 1), down)
        net.send(out, tag + "rest", src(1), ref(0, 1), up)
        net.send(out, tag + "rest", src(0), ref(0, 0), down)

    def ring_forward(out, tag, axis, base, ref):
        net.got(tag + "LA")
        net.send(out, tag + "rest", ref(3, 0), ref(3, 0), {axis: at(base, 1)})
        net.got(tag + "RB")
        net.send(out, tag + "rest", ref(1, 1), ref(1, 1), {axis: at(base, 3)})

    p1 = lambda k, h: xg.at[z, at(y, k), h]
    q1 = lambda k, h: xg.at[at(z, k), y, 2 + h]
    p2 = lambda k, h: xg.at[at(z, k), :, h]
    q2 = lambda k, h: xg.at[:, at(y, k), 2 + h]

    owner = {"I": x, "L": xl, "R": xr, "O": xo}
    half = {"A": 0, "B": 1}
    groups = (("IA", "IB"), ("LA", "RB"), ("LB", "RA"), ("OA", "OB"))

    def shard(role, core):
        return owner[role[0]] * 2 + core, half[role[1]]

    def along_x_open(tag, buf):
        net.send(tag, tag + "LA", buf.at[d, 0], buf.at[d, 0], right)
        net.send(tag, tag + "RB", buf.at[d, 1], buf.at[d, 1], left)
        net.send(tag, tag + "near", buf.at[d, 1], buf.at[d, 1], right)
        net.send(tag, tag + "near", buf.at[d, 0], buf.at[d, 0], left)
        for h in range(2):
            net.send(tag, tag + "s0", buf.at[d, h], buf.at[d, h], sib)

    def along_x_take(tag, buf, g):
        if g == 2:
            net.got(tag + "near", buf.at[0])
        if g == 3:
            net.got(tag + "far", buf.at[0])
        for role in groups[g]:
            block = buf.at[shard(role, c)]
            if g == 1:
                net.got(tag + role)
                net.send(tag, tag + "far", block, block, right if role == "LA" else left)
            net.send(tag, f"{tag}s{g}", block, block, sib)

    def sibling_has(tag, buf, g):
        net.got(f"{tag}s{g}", buf.at[0])

    def partial(i):
        b = order[i]
        wloads[i].wait()
        acc[:, :512] = jnp.dot(attn[...], wout[i % SLOTS], preferred_element_type=F32)
        if i + SLOTS < 16:
            wloads[i + SLOTS].start()
        rows = pl.ds(pl.multiple_of(t * 32, 32), 32)
        acc[rows, :512] += resid[:, block_cols(*b)].astype(F32)
        part[b[0] * 4 + b[1]] = acc[:, :512].astype(BF).reshape(4, 4, 32, 512)

    inbox = (rp, rq)

    def term(pq, k, j, h):
        return (k * 4 + j if pq == 0 else j * 4 + k), pq * 2 + h

    def sum_send(name, pq, k, j, h, slot, to):
        dev = {"y": at(y, to)} if pq == 0 else {"z": at(z, to)}
        out = "sums" if k else "sums0"
        net.send(out, f"{name}{pq}{k}", part.at[term(pq, k, j, h)], inbox[pq].at[k, slot], dev)

    def sum_open(k):
        for pq in range(2):
            sum_send("fA", pq, k, 2, 0, 0, 1)
            sum_send("fB", pq, k, 2, 1, 1, 3)
            sum_send("u", pq, k, 1, 1, 3, 1)
            sum_send("u", pq, k, 3, 0, 4, 3)

    def sum_pass(k):
        for pq in range(2):
            for name, j, h, slot, to_slot, to in (("fA", 1, 0, 0, 2, 1), ("fB", 3, 1, 1, 5, 3)):
                net.got(f"{name}{pq}{k}")
                b, rows = term(pq, k, j, h)
                part[b, rows] = (part[b, rows].astype(F32) + inbox[pq][k, slot].astype(F32)).astype(BF)
                sum_send("u", pq, k, j, h, to_slot, to)

    def sum_close(k):
        for pq in range(2):
            net.got(f"u{pq}{k}", inbox[pq].at[k, pl.ds(2, 4)])
            store, box = (sp, rp2) if pq == 0 else (sq, rq2)
            for h in range(2):
                b, rows = term(pq, k, 0, h)
                s = part[b, rows].astype(F32)
                s = s + inbox[pq][k, 2 + h].astype(F32) + inbox[pq][k, 4 + h].astype(F32)
                if k == 0:
                    res[pq * 256 + h * 128:pq * 256 + h * 128 + 128, :] = s.reshape(128, 512)
                else:
                    store[k - 1, h] = s.astype(BF)
            if k:
                dev = {"z": at(z, k)} if pq == 0 else {"y": at(y, k)}
                net.send(f"v{pq}", f"v{pq}", store.at[k - 1], box.at[k - 1], dev)

    def teacher_hidden():
        net.got("v0", rp2)
        net.got("v1", rq2)
        for pq, box in ((0, rp2), (1, rq2)):
            rows = slice(pq * 256, pq * 256 + 256)
            s = box[0].astype(F32) + box[1].astype(F32) + box[2].astype(F32)
            res[rows, :] += s.reshape(256, 512)

    def slot_of(role, core):
        return xg.at[owner[role[0]], 2 * core + half[role[1]]]

    def gate_up(g):
        @pl.loop(0, 7)
        def _(j):
            cols = pl.ds(pl.multiple_of(j * 256, 256), 256)
            total = None
            for core in (c, 1 - c):
                for role in groups[g]:
                    dd, h = shard(role, core)
                    lhs = slot_of(role, core)[...].reshape(512, 256)
                    term = jnp.dot(lhs, w1[dd, h, :, cols], preferred_element_type=F32)
                    total = term if total is None else total + term
            if g == 0:
                acc[:, cols] = total
            else:
                acc[:, cols] += total

    free_blocks = ((5, 6), (7, 9), (10, 11), (13, 14))

    def down(g, pq):
        core = c if pq == 0 else 1 - c
        b = free_blocks[g][pq]
        for i in range(2):
            dd, h = shard(groups[g][i], core)
            piece = jnp.dot(hid[...], w2[dd, h], preferred_element_type=F32)
            part[b, :, :, :, i * 256:(i + 1) * 256] = piece.astype(BF).reshape(4, 4, 32, 256)
        for j in (1, 2, 3):
            if pq == 0:
                yy = at(y, j)
                net.send("a", f"a{g}0", part.at[b, :, yy], r1.at[g, 0, j - 1], {"y": yy})
            else:
                zz = at(z, j)
                net.send("a", f"a{g}1", part.at[b, zz], r1.at[g, 1, j - 1], {"z": zz})

    own_sum = {}

    def middle(g, pq):
        net.got(f"a{g}{pq}", r1.at[g, pq])
        b = free_blocks[g][pq]
        for k in (1, 2, 3, 0):
            other = at(z if pq == 0 else y, k)
            mine = part[b, other, y] if pq == 0 else part[b, z, other]
            s = mine.astype(F32)
            for j in range(3):
                s = s + r1[g, pq, j, other].astype(F32)
            if k == 0:
                own_sum[g, pq] = s
            else:
                n = (2 * g + pq) * 3 + k - 1
                where = (n // 8, n // 4 % 2, n % 4)
                sp[where] = s.astype(BF)
                dev = {"z": other} if pq == 0 else {"y": other}
                net.send("b", f"b{g}{pq}", sp.at[where], r2.at[g, pq, k - 1], dev)

    def finish(g, pq):
        net.got(f"b{g}{pq}", r2.at[g, pq])
        s = own_sum[g, pq]
        for j in range(3):
            s = s + r2[g, pq, j].astype(F32)
        core = c if pq == 0 else 1 - c
        for i in range(2):
            dd, h = shard(groups[g][i], core)
            xin = xrow[dd * 2 + h].astype(F32)
            xg[g, 2 * pq + i, z, y] = (xin + s[:, i * 256:(i + 1) * 256]).astype(BF)
        ref = xg.at[g, pl.ds(2 * pq, 2), z, y]
        for j in (1, 2, 3):
            dev = {"y": at(y, j)} if pq == 0 else {"z": at(z, j)}
            net.send("c", f"c{g}{pq}", ref, ref, dev)

    def spread_ring(g, pq):
        pair = pl.ds(2 * pq, 2)
        if pq == 0:
            return f"d{g}0", "z", z, lambda k, h: xg.at[g, pair, at(z, k), pl.ds(2 * h, 2)]
        return f"d{g}1", "y", y, lambda k, h: xg.at[g, pair, pl.ds(2 * h, 2), at(y, k)]

    def spread_open(g, pq):
        net.got(f"c{g}{pq}", r2.at[g, pq])
        ring_open("d", *spread_ring(g, pq))

    def spread_forward(g, pq):
        ring_forward("d", *spread_ring(g, pq))

    def predict(g):
        for pq in range(2):
            net.got(f"d{g}{pq}rest", xg.at[0, 0])
        total = None
        for pq in range(2):
            core = c if pq == 0 else 1 - c
            for i in range(2):
                dd, h = shard(groups[g][i], core)
                lhs = xg[g, 2 * pq + i].reshape(512, 256)
                piece = jnp.dot(lhs, pj[dd, h], preferred_element_type=F32)
                total = piece if total is None else total + piece
        if g == 0:
            res[...] = total
        else:
            res[...] += total

    def row_squares(value):
        v = value * value
        v = v[:, 0:128] + v[:, 128:256] + v[:, 256:384] + v[:, 384:512]
        v = v.T
        parts = v[0:8, :]
        for i in range(1, 16):
            parts = parts + v[8 * i:8 * i + 8, :]
        return parts

    def stat_open(tag, own, box):
        for n, (i, j) in enumerate(others):
            net.send(tag, tag, own, box.at[n], {"z": at(z, i), "y": at(y, j)})

    def stat_take(tag, own, box):
        net.got(tag, box)
        total = own[...]
        for n in range(15):
            total = total + box[n]
        return jnp.sum(total, axis=0, keepdims=True)

    def before():
        first = lax.broadcasted_iota(jnp.int32, (512, 512), 0)
        later = lax.broadcasted_iota(jnp.int32, (512, 512), 1)
        return jnp.where(first < later, 1.0, 0.0).astype(BF)

    def dest_of(s):
        return jnp.concatenate([dest[2 * s], dest[2 * s + 1]], axis=1)

    def unpack_plan():
        for s in range(8):
            ranks[s:s + 1, :] = dest_of(s).astype(F32)
        start = (d * 512).astype(F32)
        here = ranks[...]
        here = jnp.where((here >= start) & (here < start + 512.0), 1.0, 0.0)
        rank = jnp.dot(here.astype(BF), before(), preferred_element_type=F32)
        ranks[...] = jnp.where(here > 0.0, rank, -1.0)
        row_id = d * 512 + lax.broadcasted_iota(jnp.int32, (512, 512), 0)
        slot_id = lax.broadcasted_iota(jnp.int32, (128, 512), 0).astype(F32)
        for s in range(8):
            goes = jnp.where(row_id == dest_of(s), 1.0, 0.0).astype(BF)
            takes = jnp.where(slot_id == ranks[s:s + 1, :], 1.0, 0.0).astype(BF)
            plan = lax.dot_general(goes, takes, (((1,), (1,)), ((), ())), preferred_element_type=F32)
            wout[2 + s // 4, :, (s % 4) * 128:(s % 4) * 128 + 128] = plan.astype(BF)

    def finish_target():
        scale = lax.rsqrt(stat_take("q", stat_s, stat_in) / HT + 1e-06)
        scale = jnp.broadcast_to(scale, (128, 512)).T
        eight = tgain[pl.ds(pl.multiple_of(lax.div(t, 2) * 8, 8), 8), :].astype(F32)
        four = jnp.where(lax.rem(t, 2) == 0, eight[0:4, :], eight[4:8, :])
        for r in range(4):
            for i in range(4):
                rows, cols = slice(r * 128, r * 128 + 128), slice(i * 128, i * 128 + 128)
                final = (res[rows, cols] * scale[rows, :] * four[i:i + 1, :]).astype(BF)
                rp[0, r, :, :, cols] = final.reshape(4, 32, 128)
        final = rp[0, 0:4].reshape(512, 512)
        tile = lax.shift_right_logical(dest_of(d), 9)
        is_tile = jnp.where(lax.broadcasted_iota(jnp.int32, (8, 512), 0) == tile, 1.0, 0.0)
        rank = jnp.dot(is_tile.astype(BF), before(), preferred_element_type=F32)
        slot = tile.astype(F32) * 128.0 + jnp.sum(rank * is_tile, axis=0, keepdims=True)
        slot_id = lax.broadcasted_iota(jnp.int32, (512, 512), 0).astype(F32)
        for i in range(2):
            pick = jnp.where(slot_id + 512.0 * i == slot, 1.0, 0.0).astype(BF)
            wout[i] = jnp.dot(pick, final, preferred_element_type=F32).astype(BF)

    def packed(xx, cc):
        where = (lax.rem(xx, 2) * 2 + cc) * 128
        return wout.at[lax.div(xx, 2), pl.ds(pl.multiple_of(where, 128), 128)]

    def target_open():
        for k, far in ((2, 0), (2, 1), (1, 0), (3, 0), (1, 1), (3, 1), (0, 1)):
            xx, cc = at(x, k), (1 - c if far else c)
            net.send("t", "t", packed(xx, cc), ta.at[d], {"x": xx, "c": cc})
        ta[d] = packed(x, c)[...]

    def subtract_target():
        net.got("t", ta.at[pl.ds(0, 7)])
        for i in range(2):
            rows = ta[4 * i:4 * i + 4].reshape(512, 512)
            res[...] -= jnp.dot(wout[2 + i], rows, preferred_element_type=F32)

    def both(step, g):
        step(g, 0)
        step(g, 1)

    def downs(g):
        down(g, 0)
        sibling_has("m", w2, g)
        down(g, 1)

    ring_open("near", "p1", "y", y, p1, lambda h: sin.at[h])
    ring_open("near", "q1", "z", z, q1, lambda h: sin.at[2 + h])
    for cp in loads[:4]:
        cp.wait()
    along_x_open("w", w1)
    for i in range(SLOTS):
        wloads[i].start()
    for cp in w2_loads + pj_loads:
        cp.start()
    for i in range(5):
        partial(i)
    ring_forward("near", "p1", "y", y, p1)
    ring_forward("near", "q1", "z", z, q1)
    sum_open(1)
    partial(5)
    partial(6)
    loads[4].wait()
    net.got("p1rest", xg.at[0, 0])
    ring_open("wide", "p2", "z", z, p2)
    net.got("q1rest", xg.at[0, 0])
    ring_open("wide", "q2", "y", y, q2)
    partial(7)
    partial(8)
    sum_pass(1)
    for i in range(9, 16):
        partial(i)
    sum_open(2)
    ring_forward("wide", "p2", "z", z, p2)
    ring_forward("wide", "q2", "y", y, q2)
    sum_open(3)
    along_x_take("w", w1, 1)
    for cp in w2_loads:
        cp.wait()
    along_x_open("m", w2)
    sum_pass(2)
    sum_open(0)
    unpack_plan()
    net.got("p2rest", xg.at[0])
    net.got("q2rest", xg.at[0])
    net.flush("near", xg.at[0, pl.ds(0, 3)])
    net.flush("wide", xg.at[pl.ds(0, 3)])
    xrow[...] = xg[:, :, z, y].reshape(16, 32, 256)

    @pl.loop(0, 4)
    def _(r):
        total = jnp.zeros((128, 256), F32)
        for s in range(16):
            v = xg[s // 4, s % 4, r].reshape(128, 256).astype(F32)
            total = total + v * v
        scale = lax.rsqrt(jnp.sum(total, axis=1, keepdims=True) / 4096.0 + 1e-05)
        for s in range(16):
            v = xg[s // 4, s % 4, r].reshape(128, 256).astype(F32)
            g = jnp.concatenate([gain[2 * s:2 * s + 1, :], gain[2 * s + 1:2 * s + 2, :]], axis=1)
            xg[s // 4, s % 4, r] = (v * scale * g.astype(F32)).astype(BF).reshape(4, 32, 256)

    sum_pass(3)
    sibling_has("w", w1, 0)
    gate_up(0)
    sum_close(1)
    sibling_has("w", w1, 1)
    gate_up(1)
    along_x_take("w", w1, 2)
    sum_pass(0)
    sum_close(2)
    sibling_has("w", w1, 2)
    gate_up(2)
    sum_close(3)
    along_x_take("w", w1, 3)
    sibling_has("w", w1, 3)
    gate_up(3)

    @pl.loop(0, 7)
    def _(j):
        g = acc[:, pl.ds(pl.multiple_of(j * 128, 128), 128)]
        u = acc[:, pl.ds(pl.multiple_of(896 + j * 128, 128), 128)]
        hid[:, pl.ds(pl.multiple_of(j * 128, 128), 128)] = (jax.nn.silu(g) * u).astype(BF)

    net.flush("sums", part.at[pl.ds(0, 9)])
    net.flush("v0", sp)
    downs(0)
    for cp in pj_loads:
        cp.wait()
    sum_close(0)
    along_x_take("m", w2, 1)
    along_x_open("p", pj)
    downs(1)
    both(middle, 0)
    teacher_hidden()
    stat_s[...] = row_squares(res[...])
    pl.semaphore_wait(plane, 3)
    stat_open("q", stat_s, stat_in)
    both(middle, 1)
    both(finish, 0)
    along_x_take("m", w2, 2)
    downs(2)
    both(finish, 1)
    both(spread_open, 0)
    finish_target()
    target_open()
    both(middle, 2)
    along_x_take("m", w2, 3)
    downs(3)
    both(spread_open, 1)
    both(spread_forward, 0)
    both(finish, 2)
    along_x_take("p", pj, 1)
    both(middle, 3)
    along_x_take("p", pj, 2)
    both(spread_forward, 1)
    both(spread_open, 2)
    sibling_has("p", pj, 0)
    predict(0)
    both(finish, 3)
    along_x_take("p", pj, 3)
    both(spread_forward, 2)
    sibling_has("p", pj, 1)
    predict(1)
    both(spread_open, 3)
    both(spread_forward, 3)
    sibling_has("p", pj, 2)
    predict(2)
    subtract_target()
    sibling_has("p", pj, 3)
    predict(3)

    h0 = lax.rem(t, 2)
    d0 = lax.div(t, 2)
    k0 = lax.rem(lax.div(d0, 2) - x + 4, 4)
    k_odd, k_two = lax.rem(k0, 2), lax.div(k0, 2)
    g0 = (1 - k_odd) * k_two * 3 + k_odd * (k_two * (1 + h0) + (1 - k_two) * (2 - h0))
    i0 = (1 - k_odd) * h0 + k_odd * (1 - k_two)
    out[...] = xg[g0, 2 * lax.rem(d0 + c, 2) + i0].reshape(512, 256)

    loss_s[...] = row_squares(res[...])
    stat_open("l", loss_s, loss_in)
    loss[...] = stat_take("l", loss_s, loss_in) / HT
    for out_tag, ref in (
        ("w", w1.at[pl.ds(0, 7)]), ("m", w2.at[pl.ds(0, 7)]), ("p", pj.at[pl.ds(0, 7)]),
        ("t", ta.at[pl.ds(0, 7)]), ("sums0", part.at[pl.ds(0, 3)]), ("v1", sq), ("a", part.at[pl.ds(0, 6)]),
        ("b", r2), ("c", r2), ("d", xg.at[pl.ds(0, 3)]), ("q", stat_in), ("l", loss_in),
    ):
        net.flush(out_tag, ref)


def call_kernel(*args):
    vm = pl.BlockSpec(memory_space=pltpu.VMEM)
    hb = pl.BlockSpec(memory_space=pl.ANY)
    return pl.pallas_call(
        kernel,
        name="first",
        out_shape=(
            jax.ShapeDtypeStruct((512, 256), BF),
            jax.ShapeDtypeStruct((512, 512), F32),
            jax.ShapeDtypeStruct((1, 512), F32),
        ),
        in_specs=[vm, hb, vm, vm, vm, hb, hb, hb, hb, vm, vm],
        out_specs=(vm, vm, vm),
        scratch_shapes=[
            pltpu.VMEM((8, 2, 256, 1792), BF),
            pltpu.VMEM((4, 4, 4, 4, 32, 256), BF),
            pltpu.VMEM((4, 512, 512), BF),
            pltpu.VMEM((16, 4, 4, 32, 512), BF),
            pltpu.VMEM((4, 6, 4, 32, 512), BF),
            pltpu.VMEM((4, 6, 4, 32, 512), BF),
            pltpu.VMEM((3, 2, 4, 32, 512), BF),
            pltpu.VMEM((3, 2, 4, 32, 512), BF),
            pltpu.VMEM((3, 2, 4, 32, 512), BF),
            pltpu.VMEM((3, 2, 4, 32, 512), BF),
            pltpu.VMEM((512, 1792), F32),
            pltpu.VMEM((512, 896), BF),
            pltpu.VMEM((16, 32, 256), BF),
            pltpu.VMEM((8, 2, 896, 256), BF),
            pltpu.VMEM((8, 2, 256, 512), BF),
            pltpu.VMEM((4, 2, 3, 4, 32, 512), BF),
            pltpu.VMEM((4, 2, 3, 32, 512), BF),
            pltpu.VMEM((15, 8, 512), F32),
            pltpu.VMEM((8, 512), F32),
            pltpu.VMEM((15, 8, 512), F32),
            pltpu.VMEM((8, 512), F32),
            pltpu.VMEM((8, 512), F32),
            pltpu.VMEM((8, 128, 512), BF),
            pltpu.SemaphoreType.DMA((9,)),
            pltpu.SemaphoreType.DMA((4,)),
            pltpu.SemaphoreType.REGULAR,
            pltpu.SemaphoreType.DMA((SENDS,)),
            pltpu.SemaphoreType.DMA((RECEIVES,)),
        ],
        compiler_params=pltpu.CompilerParams(
            collective_id=0, has_side_effects=True, vmem_limit_bytes=67043328
        ),
    )(*args)


def keep(out, res, loss, out_to, res_to, loss_to):
    out_to[...] = out[...]
    res_to[...] = res[...]
    loss_to[...] = loss[...]


def local(
    attn_ctx,
    w_out,
    resid,
    teacher_gain,
    dest_row,
    student_in,
    student_gain,
    w_gate,
    w_up,
    w_down,
    proj,
):
    made = call_kernel(
        attn_ctx,
        w_out,
        resid,
        student_in.reshape(4, 4, 32, 256),
        student_gain.reshape(32, 128),
        w_gate,
        w_up,
        w_down,
        proj,
        teacher_gain.reshape(64, 128),
        dest_row.reshape(16, 1, 256),
    )
    vm = pl.BlockSpec(memory_space=pltpu.VMEM)
    out, residue, loss = pl.pallas_call(
        keep,
        name="keep",
        out_shape=tuple(jax.ShapeDtypeStruct(a.shape, a.dtype) for a in made),
        in_specs=[vm, vm, vm],
        out_specs=(vm, vm, vm),
    )(*made)
    return (out, loss.reshape(512), residue)


def solution(mesh):
    torus = Mesh(mesh.devices.reshape(4, 2, 4, 4), AXES)
    in_specs = (
        P(DP, TENSOR),
        P(TENSOR, None),
        P(DP + TENSOR, None),
        P(),
        P(),
        P(DP, TENSOR),
        P(),
        P(DP, TENSOR),
        P(DP, TENSOR),
        P(TENSOR, DP),
        P(DP, TENSOR),
    )
    out_specs = (P(DP, TENSOR), P(DP), P(DP, TENSOR))
    return jax.shard_map(local, mesh=torus, in_specs=in_specs, out_specs=out_specs, check_vma=False)
```

```python
import jax
import jax.numpy as jnp
from jax import lax
from jax.sharding import Mesh
from jax.sharding import PartitionSpec as P
from jax.experimental import pallas as pl
from jax.experimental.pallas import tpu as pltpu

HT = 8192
BF = jnp.bfloat16
F32 = jnp.float32
AXES = ("x", "c", "z", "y")
TENSOR = ("z", "y")
DP = ("x", "c")
SENDS, RECEIVES = 16, 129


class Net:
    def __init__(self, send_sems, recv_sems):
        self.ss, self.rs, self.sent, self.due, self.made = send_sems, recv_sems, {}, {}, {}

    def send(self, out, role, src, dst, dev):
        i = self.sent.setdefault(out, len(self.sent))
        j = self.due.setdefault(role, len(self.due))
        cp = pltpu.make_async_remote_copy(
            src_ref=src,
            dst_ref=dst,
            send_sem=self.ss.at[i],
            recv_sem=self.rs.at[j],
            device_id=dev,
            device_id_type=pl.DeviceIdType.MESH,
        )
        cp.start()
        self.made[role] = cp

    def got(self, role, bytes_of=None):
        if bytes_of is None:
            self.made[role].wait_recv()
        else:
            pltpu.make_async_copy(bytes_of, bytes_of, self.rs.at[self.due[role]]).wait()

    def flush(self, out, bytes_of):
        pltpu.make_async_copy(bytes_of, bytes_of, self.ss.at[self.sent[out]]).wait()


def greet(partners):
    barrier = pltpu.get_barrier_semaphore()
    for dev in partners:
        pl.semaphore_signal(barrier, inc=1, device_id=dev, device_id_type=pl.DeviceIdType.MESH)
    pl.semaphore_wait(barrier, len(partners))


def kernel(
    attn, wout_hbm, resid, sin, gain, wg_hbm, wu_hbm, wd_hbm, pj_hbm, tgain, dest,
    out, res_out, loss,
    res, w1, xg, wout, part, rp, rq, sp, sq, rp2, rq2, acc, hid, xrow, w2, pj, r1, r2,
    stat_in, stat_s, loss_in, loss_s, ranks, ta, loc, wsem, plane, ss, rs,
):
    x, c, z, y = (lax.axis_index(a) for a in AXES)
    t = z * 4 + y
    d = x * 2 + c

    def at(base, k):
        return lax.rem(base + k, 4)

    xr, xl, xo = at(x, 1), at(x, 3), at(x, 2)
    sib = {"c": 1 - c}
    right, left = {"x": xr}, {"x": xl}
    loads, w2_loads, pj_loads = [], [], []
    for h in range(2):
        rows = pl.ds(h * 256, 256)
        loads.append(pltpu.make_async_copy(wg_hbm.at[rows], w1.at[d, h, :, pl.ds(0, 896)], loc.at[2 * h]))
        loads.append(pltpu.make_async_copy(wu_hbm.at[rows], w1.at[d, h, :, pl.ds(896, 896)], loc.at[2 * h + 1]))
        w2_loads.append(pltpu.make_async_copy(wd_hbm.at[:, rows], w2.at[d, h], loc.at[5 + h]))
        pj_loads.append(pltpu.make_async_copy(pj_hbm.at[rows], pj.at[d, h], loc.at[7 + h]))
    loads.append(pltpu.make_async_copy(sin, xg.at[z, y], loc.at[4]))
    for cp in loads:
        cp.start()

    order = (
        (1, 1), (1, 2), (2, 1), (1, 3), (3, 1), (2, 2), (2, 3), (3, 2), (3, 3),
        (0, 1), (1, 0), (0, 2), (2, 0), (0, 3), (3, 0), (0, 0),
    )
    SLOTS = 4

    def block_cols(dz, dy):
        return pl.ds(pl.multiple_of((at(z, dz) * 4 + at(y, dy)) * 512, 512), 512)

    wloads = [
        pltpu.make_async_copy(wout_hbm.at[:, block_cols(*b)], wout.at[i % SLOTS], wsem.at[i % SLOTS])
        for i, b in enumerate(order)
    ]

    others = [(i, j) for i in range(4) for j in range(4) if (i, j) != (0, 0)]
    greet([sib, right, left] + [{a: at(b, k)} for a, b in (("y", y), ("z", z)) for k in (1, 2, 3)])
    net = Net(ss, rs)
    for k in (1, 2, 3):
        pl.semaphore_signal(plane, inc=1, device_id={"y": at(y, k)}, device_id_type=pl.DeviceIdType.MESH)

    def ring_open(out, tag, axis, base, ref, src=None):
        up, down = {axis: at(base, 1)}, {axis: at(base, 3)}
        src = src or (lambda h: ref(0, h))
        net.send(out, tag + "LA", src(0), ref(0, 0), up)
        net.send(out, tag + "RB", src(1), ref(0, 1), down)
        net.send(out, tag + "rest", src(1), ref(0, 1), up)
        net.send(out, tag + "rest", src(0), ref(0, 0), down)

    def ring_forward(out, tag, axis, base, ref):
        net.got(tag + "LA")
        net.send(out, tag + "rest", ref(3, 0), ref(3, 0), {axis: at(base, 1)})
        net.got(tag + "RB")
        net.send(out, tag + "rest", ref(1, 1), ref(1, 1), {axis: at(base, 3)})

    p1 = lambda k, h: xg.at[z, at(y, k), h]
    q1 = lambda k, h: xg.at[at(z, k), y, 2 + h]
    p2 = lambda k, h: xg.at[at(z, k), :, h]
    q2 = lambda k, h: xg.at[:, at(y, k), 2 + h]

    owner = {"I": x, "L": xl, "R": xr, "O": xo}
    half = {"A": 0, "B": 1}
    groups = (("IA", "IB"), ("LA", "RB"), ("LB", "RA"), ("OA", "OB"))

    def shard(role, core):
        return owner[role[0]] * 2 + core, half[role[1]]

    def along_x_open(tag, buf):
        net.send(tag, tag + "LA", buf.at[d, 0], buf.at[d, 0], right)
        net.send(tag, tag + "RB", buf.at[d, 1], buf.at[d, 1], left)
        net.send(tag, tag + "near", buf.at[d, 1], buf.at[d, 1], right)
        net.send(tag, tag + "near", buf.at[d, 0], buf.at[d, 0], left)
        for h in range(2):
            net.send(tag, tag + "s0", buf.at[d, h], buf.at[d, h], sib)

    quarters = (pl.ds(0, 128), pl.ds(128, 128))

    def w1_forward():
        for i, rows in enumerate(quarters):
            for role, dev in (("LA", right), ("RB", left)):
                if i == 0:
                    net.got("w" + role)
                block = w1.at[shard(role, c) + (rows,)]
                net.send("w", f"wfar{i}", block, block, dev)
        for role in groups[1]:
            block = w1.at[shard(role, c)]
            net.send("w", "ws1", block, block, sib)

    def w2_forward():
        for u, cols in enumerate(quarters):
            for role, dev in (("LA", right), ("RB", left)):
                if u == 0:
                    net.got("m" + role)
                block = w2.at[shard(role, c) + (slice(None), cols)]
                net.send("m", f"mfar{u}", block, block, dev)
        for role in groups[1]:
            block = w2.at[shard(role, c)]
            net.send("m", "ms1", block, block, sib)

    def w2_far(u):
        net.got(f"mfar{u}", w2.at[0, 0])
        for role in groups[3]:
            block = w2.at[shard(role, c) + (slice(None), quarters[u])]
            net.send("m", f"ms3{u}", block, block, sib)

    def w1_far(i):
        net.got(f"wfar{i}", w1.at[0, 0])
        for role in groups[3]:
            block = w1.at[shard(role, c) + (quarters[i],)]
            net.send("w", f"ws3{i}", block, block, sib)

    def along_x_take(tag, buf, g):
        if g == 2:
            net.got(tag + "near", buf.at[0])
        if g == 3:
            net.got(tag + "far", buf.at[0])
        for role in groups[g]:
            block = buf.at[shard(role, c)]
            if g == 1:
                net.got(tag + role)
                net.send(tag, tag + "far", block, block, right if role == "LA" else left)
            net.send(tag, f"{tag}s{g}", block, block, sib)

    def sibling_has(tag, buf, g):
        net.got(f"{tag}s{g}", buf.at[0])

    def partial(i):
        b = order[i]
        wloads[i].wait()
        acc[:, :512] = jnp.dot(attn[...], wout[i % SLOTS], preferred_element_type=F32)
        if i + SLOTS < 16:
            wloads[i + SLOTS].start()
        rows = pl.ds(pl.multiple_of(t * 32, 32), 32)
        acc[rows, :512] += resid[:, block_cols(*b)].astype(F32)
        part[b[0] * 4 + b[1]] = acc[:, :512].astype(BF).reshape(4, 4, 32, 512)

    inbox = (rp, rq)

    def term(pq, k, j, h):
        return (k * 4 + j if pq == 0 else j * 4 + k), pq * 2 + h

    def sum_send(name, pq, k, j, h, slot, to):
        dev = {"y": at(y, to)} if pq == 0 else {"z": at(z, to)}
        out = "sums" if k else "sums0"
        net.send(out, f"{name}{pq}{k}", part.at[term(pq, k, j, h)], inbox[pq].at[k, slot], dev)

    def sum_open(k):
        for pq in range(2):
            sum_send("fA", pq, k, 2, 0, 0, 1)
            sum_send("fB", pq, k, 2, 1, 1, 3)
            sum_send("u", pq, k, 1, 1, 3, 1)
            sum_send("u", pq, k, 3, 0, 4, 3)

    def sum_pass(k):
        for pq in range(2):
            for name, j, h, slot, to_slot, to in (("fA", 1, 0, 0, 2, 1), ("fB", 3, 1, 1, 5, 3)):
                net.got(f"{name}{pq}{k}")
                b, rows = term(pq, k, j, h)
                part[b, rows] = (part[b, rows].astype(F32) + inbox[pq][k, slot].astype(F32)).astype(BF)
                sum_send("u", pq, k, j, h, to_slot, to)

    def sum_close(k):
        for pq in range(2):
            net.got(f"u{pq}{k}", inbox[pq].at[k, pl.ds(2, 4)])
            store, box = (sp, rp2) if pq == 0 else (sq, rq2)
            for h in range(2):
                b, rows = term(pq, k, 0, h)
                s = part[b, rows].astype(F32)
                s = s + inbox[pq][k, 2 + h].astype(F32) + inbox[pq][k, 4 + h].astype(F32)
                if k == 0:
                    res[pq * 256 + h * 128:pq * 256 + h * 128 + 128, :] = s.reshape(128, 512)
                else:
                    store[k - 1, h] = s.astype(BF)
            if k:
                dev = {"z": at(z, k)} if pq == 0 else {"y": at(y, k)}
                net.send(f"v{pq}", f"v{pq}", store.at[k - 1], box.at[k - 1], dev)

    def teacher_hidden():
        net.got("v0", rp2)
        net.got("v1", rq2)
        for pq, box in ((0, rp2), (1, rq2)):
            rows = slice(pq * 256, pq * 256 + 256)
            s = box[0].astype(F32) + box[1].astype(F32) + box[2].astype(F32)
            res[rows, :] += s.reshape(256, 512)

    def slot_of(role, core):
        return xg.at[owner[role[0]], 2 * core + half[role[1]]]

    def gate_up(g, i=None):
        @pl.loop(0, 7)
        def _(j):
            cols = pl.ds(pl.multiple_of(j * 256, 256), 256)
            total = None
            for core in (c, 1 - c):
                both_roles = [(slot_of(role, core), w1.at[shard(role, core)]) for role in groups[g]]
                if i is None:
                    pairs = [(lhs[...].reshape(512, 256), rhs[:, cols]) for lhs, rhs in both_roles]
                else:
                    part_of = slice(i * 128, i * 128 + 128)
                    lhs = [lhs[..., part_of].reshape(512, 128) for lhs, rhs in both_roles]
                    rhs = [rhs[part_of, cols] for lhs_, rhs in both_roles]
                    pairs = [(jnp.concatenate(lhs, axis=1), jnp.concatenate(rhs, axis=0))]
                for lhs, rhs in pairs:
                    piece = jnp.dot(lhs, rhs, preferred_element_type=F32)
                    total = piece if total is None else total + piece
            if g == 0:
                acc[:, cols] = total
            else:
                acc[:, cols] += total

    steps = ((0, (0, 1)), (1, (0, 1)), (2, (0, 1)), (3, (0,)), (3, (1,)))
    free_blocks = ((5, 6), (7, 9), (10, 11), (13, 14))

    def pieces(g, pq):
        return [shard(role, c if pq == 0 else 1 - c) for role in groups[g]]

    def lanes_of(n):
        us = steps[n][1]
        return pl.ds(us[0] * 256, len(us) * 256)

    def down(n, pq):
        g, us = steps[n]
        b = free_blocks[g][pq]
        lanes = lanes_of(n)
        for u in us:
            cut = slice(u * 128, u * 128 + 128)
            rhs = jnp.concatenate([w2[dd, h, :, cut] for dd, h in pieces(g, pq)], axis=1)
            piece = jnp.dot(hid[...], rhs, preferred_element_type=F32)
            part[b, :, :, :, u * 256:(u + 1) * 256] = piece.astype(BF).reshape(4, 4, 32, 256)
        for j in (1, 2, 3):
            to = r1.at[g, pq, j - 1, :, :, lanes]
            if pq == 0:
                yy = at(y, j)
                net.send("a", f"a{n}0", part.at[b, :, yy, :, lanes], to, {"y": yy})
            else:
                zz = at(z, j)
                net.send("a", f"a{n}1", part.at[b, zz, :, :, lanes], to, {"z": zz})

    own_sum = {}

    def middle(n, pq):
        g, us = steps[n]
        lanes = lanes_of(n)
        net.got(f"a{n}{pq}", r1.at[g, pq, :, :, :, lanes])
        b = free_blocks[g][pq]
        for k in (1, 2, 3, 0):
            other = at(z if pq == 0 else y, k)
            mine = part[b, other, y, :, lanes] if pq == 0 else part[b, z, other, :, lanes]
            s = mine.astype(F32)
            for j in range(3):
                s = s + r1[g, pq, j, other, :, lanes].astype(F32)
            if k == 0:
                own_sum[n, pq] = s
            else:
                i = (2 * g + pq) * 3 + k - 1
                where = (i // 8, i // 4 % 2, i % 4, slice(None), lanes)
                sp[where] = s.astype(BF)
                dev = {"z": other} if pq == 0 else {"y": other}
                net.send("b", f"b{n}{pq}", sp.at[where], r2.at[g, pq, k - 1, :, lanes], dev)

    def finish(n, pq):
        g, us = steps[n]
        lanes = lanes_of(n)
        net.got(f"b{n}{pq}", r2.at[g, pq, :, :, lanes])
        s = own_sum[n, pq]
        for j in range(3):
            s = s + r2[g, pq, j, :, lanes].astype(F32)
        for i, u in enumerate(us):
            cut = slice(u * 128, u * 128 + 128)
            xin = jnp.concatenate([xrow[dd * 2 + h, :, cut] for dd, h in pieces(g, pq)], axis=1)
            mlp = s[:, i * 256:(i + 1) * 256]
            xg[g, 2 * pq + u, z, y] = (xin.astype(F32) + mlp).astype(BF)
        ref = xg.at[g, pl.ds(2 * pq + us[0], len(us)), z, y]
        for j in (1, 2, 3):
            dev = {"y": at(y, j)} if pq == 0 else {"z": at(z, j)}
            net.send("c", f"c{n}{pq}", ref, ref, dev)

    def spread_ring(n, pq):
        g, us = steps[n]
        pair = pl.ds(2 * pq + us[0], len(us))
        if pq == 0:
            return f"d{n}0", "z", z, lambda k, h: xg.at[g, pair, at(z, k), pl.ds(2 * h, 2)]
        return f"d{n}1", "y", y, lambda k, h: xg.at[g, pair, pl.ds(2 * h, 2), at(y, k)]

    def spread_open(n, pq):
        g, us = steps[n]
        net.got(f"c{n}{pq}", r2.at[g, pq, :, :, lanes_of(n)])
        ring_open("d", *spread_ring(n, pq))

    def spread_forward(n, pq):
        ring_forward("d", *spread_ring(n, pq))

    def spread_close(n):
        for pq in range(2):
            net.got(f"d{n}{pq}rest", xg.at[0, 0, pl.ds(0, 2 * len(steps[n][1]))])

    def predict(n, first=False):
        g, us = steps[n]
        total = None
        for pq in range(2):
            for u in us:
                cut = slice(u * 128, u * 128 + 128)
                rhs = jnp.concatenate([pj[dd, h, cut, :] for dd, h in pieces(g, pq)], axis=0)
                lhs = xg[g, 2 * pq + u].reshape(512, 256)
                piece = jnp.dot(lhs, rhs, preferred_element_type=F32)
                total = piece if total is None else total + piece
        if first:
            res[...] = total
        else:
            res[...] += total

    def row_squares(value):
        v = value * value
        v = v[:, 0:128] + v[:, 128:256] + v[:, 256:384] + v[:, 384:512]
        v = v.T
        parts = v[0:8, :]
        for i in range(1, 16):
            parts = parts + v[8 * i:8 * i + 8, :]
        return parts

    def stat_open(tag, own, box):
        for n, (i, j) in enumerate(others):
            net.send(tag, tag, own, box.at[n], {"z": at(z, i), "y": at(y, j)})

    def stat_take(tag, own, box):
        net.got(tag, box)
        total = own[...]
        for n in range(15):
            total = total + box[n]
        return jnp.sum(total, axis=0, keepdims=True)

    def before():
        first = lax.broadcasted_iota(jnp.int32, (512, 512), 0)
        later = lax.broadcasted_iota(jnp.int32, (512, 512), 1)
        return jnp.where(first < later, 1.0, 0.0).astype(BF)

    def dest_of(s):
        return jnp.concatenate([dest[2 * s], dest[2 * s + 1]], axis=1)

    def unpack_plan():
        for s in range(8):
            ranks[s:s + 1, :] = dest_of(s).astype(F32)
        start = (d * 512).astype(F32)
        here = ranks[...]
        here = jnp.where((here >= start) & (here < start + 512.0), 1.0, 0.0)
        rank = jnp.dot(here.astype(BF), before(), preferred_element_type=F32)
        ranks[...] = jnp.where(here > 0.0, rank, -1.0)
        row_id = d * 512 + lax.broadcasted_iota(jnp.int32, (512, 512), 0)
        slot_id = lax.broadcasted_iota(jnp.int32, (128, 512), 0).astype(F32)
        for s in range(8):
            goes = jnp.where(row_id == dest_of(s), 1.0, 0.0).astype(BF)
            takes = jnp.where(slot_id == ranks[s:s + 1, :], 1.0, 0.0).astype(BF)
            plan = lax.dot_general(goes, takes, (((1,), (1,)), ((), ())), preferred_element_type=F32)
            wout[2 + s // 4, :, (s % 4) * 128:(s % 4) * 128 + 128] = plan.astype(BF)

    def finish_target():
        scale = lax.rsqrt(stat_take("q", stat_s, stat_in) / HT + 1e-06)
        scale = jnp.broadcast_to(scale, (128, 512)).T
        eight = tgain[pl.ds(pl.multiple_of(lax.div(t, 2) * 8, 8), 8), :].astype(F32)
        four = jnp.where(lax.rem(t, 2) == 0, eight[0:4, :], eight[4:8, :])
        for r in range(4):
            for i in range(4):
                rows, cols = slice(r * 128, r * 128 + 128), slice(i * 128, i * 128 + 128)
                final = (res[rows, cols] * scale[rows, :] * four[i:i + 1, :]).astype(BF)
                rp[0, r, :, :, cols] = final.reshape(4, 32, 128)
        final = rp[0, 0:4].reshape(512, 512)
        tile = lax.shift_right_logical(dest_of(d), 9)
        is_tile = jnp.where(lax.broadcasted_iota(jnp.int32, (8, 512), 0) == tile, 1.0, 0.0)
        rank = jnp.dot(is_tile.astype(BF), before(), preferred_element_type=F32)
        slot = tile.astype(F32) * 128.0 + jnp.sum(rank * is_tile, axis=0, keepdims=True)
        slot_id = lax.broadcasted_iota(jnp.int32, (512, 512), 0).astype(F32)
        for i in range(2):
            pick = jnp.where(slot_id + 512.0 * i == slot, 1.0, 0.0).astype(BF)
            wout[i] = jnp.dot(pick, final, preferred_element_type=F32).astype(BF)

    def packed(xx, cc):
        where = (lax.rem(xx, 2) * 2 + cc) * 128
        return wout.at[lax.div(xx, 2), pl.ds(pl.multiple_of(where, 128), 128)]

    def target_open():
        for k, far in ((2, 0), (2, 1), (1, 0), (3, 0), (1, 1), (3, 1), (0, 1)):
            xx, cc = at(x, k), (1 - c if far else c)
            net.send("t", "t", packed(xx, cc), ta.at[d], {"x": xx, "c": cc})
        ta[d] = packed(x, c)[...]

    def subtract_target():
        net.got("t", ta.at[pl.ds(0, 7)])
        for i in range(2):
            rows = ta[4 * i:4 * i + 4].reshape(512, 512)
            res[...] -= jnp.dot(wout[2 + i], rows, preferred_element_type=F32)

    def both(step, g):
        step(g, 0)
        step(g, 1)

    def downs(n):
        down(n, 0)
        if n < 3:
            sibling_has("m", w2, n)
        else:
            net.got(f"ms3{n - 3}", w2.at[0, 0])
        down(n, 1)

    ring_open("near", "p1", "y", y, p1, lambda h: sin.at[h])
    ring_open("near", "q1", "z", z, q1, lambda h: sin.at[2 + h])
    for cp in loads[:4]:
        cp.wait()
    along_x_open("w", w1)
    for i in range(SLOTS):
        wloads[i].start()
    for cp in w2_loads + pj_loads:
        cp.start()
    for i in range(5):
        partial(i)
    ring_forward("near", "p1", "y", y, p1)
    ring_forward("near", "q1", "z", z, q1)
    sum_open(1)
    partial(5)
    partial(6)
    loads[4].wait()
    net.got("p1rest", xg.at[0, 0])
    ring_open("wide", "p2", "z", z, p2)
    net.got("q1rest", xg.at[0, 0])
    ring_open("wide", "q2", "y", y, q2)
    partial(7)
    partial(8)
    sum_pass(1)
    for i in range(9, 16):
        partial(i)
    sum_open(2)
    ring_forward("wide", "p2", "z", z, p2)
    ring_forward("wide", "q2", "y", y, q2)
    sum_open(3)
    w1_forward()
    for cp in w2_loads:
        cp.wait()
    along_x_open("m", w2)
    sum_pass(2)
    sum_open(0)
    unpack_plan()
    net.got("p2rest", xg.at[0])
    net.got("q2rest", xg.at[0])
    net.flush("near", xg.at[0, pl.ds(0, 3)])
    net.flush("wide", xg.at[pl.ds(0, 3)])
    xrow[...] = xg[:, :, z, y].reshape(16, 32, 256)

    @pl.loop(0, 4)
    def _(r):
        total = jnp.zeros((128, 256), F32)
        for s in range(16):
            v = xg[s // 4, s % 4, r].reshape(128, 256).astype(F32)
            total = total + v * v
        scale = lax.rsqrt(jnp.sum(total, axis=1, keepdims=True) / 4096.0 + 1e-05)
        for s in range(16):
            v = xg[s // 4, s % 4, r].reshape(128, 256).astype(F32)
            g = jnp.concatenate([gain[2 * s:2 * s + 1, :], gain[2 * s + 1:2 * s + 2, :]], axis=1)
            xg[s // 4, s % 4, r] = (v * scale * g.astype(F32)).astype(BF).reshape(4, 32, 256)

    sum_pass(3)
    sibling_has("w", w1, 0)
    gate_up(0)
    sum_close(1)
    sibling_has("w", w1, 1)
    gate_up(1)
    along_x_take("w", w1, 2)
    sum_pass(0)
    sum_close(2)
    sibling_has("w", w1, 2)
    gate_up(2)
    sum_close(3)
    for i in range(2):
        w1_far(i)
        net.got(f"ws3{i}", w1.at[0, 0])
        gate_up(3, i)

    @pl.loop(0, 7)
    def _(j):
        g = acc[:, pl.ds(pl.multiple_of(j * 128, 128), 128)]
        u = acc[:, pl.ds(pl.multiple_of(896 + j * 128, 128), 128)]
        hid[:, pl.ds(pl.multiple_of(j * 128, 128), 128)] = (jax.nn.silu(g) * u).astype(BF)

    net.flush("sums", part.at[pl.ds(0, 9)])
    net.flush("v0", sp)
    sibling_has("m", w2, 0)
    down(0, 1)
    down(0, 0)
    w2_forward()
    sibling_has("m", w2, 1)
    down(1, 1)
    sum_close(0)
    teacher_hidden()
    stat_s[...] = row_squares(res[...])
    pl.semaphore_wait(plane, 3)
    stat_open("q", stat_s, stat_in)
    down(1, 0)
    along_x_take("m", w2, 2)
    middle(0, 1)
    down(2, 0)
    middle(0, 0)
    sibling_has("m", w2, 2)
    down(2, 1)
    for cp in pj_loads:
        cp.wait()
    along_x_open("p", pj)
    finish(0, 0)
    finish(0, 1)
    w2_far(0)
    middle(1, 1)
    finish_target()
    target_open()
    net.got("ms30", w2.at[0, 0])
    down(3, 1)
    w2_far(1)
    middle(1, 0)
    down(3, 0)
    middle(2, 1)
    net.got("ms31", w2.at[0, 0])
    down(4, 1)
    down(4, 0)
    spread_open(0, 1)
    finish(1, 1)
    middle(3, 1)
    middle(2, 0)
    middle(3, 0)
    finish(1, 0)
    spread_open(0, 0)
    finish(2, 1)
    middle(4, 1)
    spread_forward(0, 1)
    middle(4, 0)
    finish(2, 0)
    finish(3, 0)
    along_x_take("p", pj, 1)
    spread_forward(0, 0)
    finish(3, 1)
    spread_open(1, 0)
    spread_open(1, 1)
    finish(4, 0)
    finish(4, 1)
    sibling_has("p", pj, 0)
    spread_close(0)
    predict(0, True)
    spread_open(2, 1)
    spread_open(2, 0)
    subtract_target()
    along_x_take("p", pj, 2)
    spread_open(3, 0)
    spread_open(3, 1)
    spread_open(4, 0)
    spread_open(4, 1)
    spread_forward(2, 1)
    spread_forward(2, 0)
    spread_forward(1, 0)
    spread_forward(1, 1)
    spread_forward(3, 1)
    spread_forward(3, 0)
    spread_forward(4, 1)
    along_x_take("p", pj, 3)
    spread_forward(4, 0)
    sibling_has("p", pj, 2)
    spread_close(2)
    predict(2)
    sibling_has("p", pj, 1)
    spread_close(1)
    predict(1)
    sibling_has("p", pj, 3)
    spread_close(3)
    predict(3)

    h0 = lax.rem(t, 2)
    d0 = lax.div(t, 2)
    k0 = lax.rem(lax.div(d0, 2) - x + 4, 4)
    k_odd, k_two = lax.rem(k0, 2), lax.div(k0, 2)
    g0 = (1 - k_odd) * k_two * 3 + k_odd * (k_two * (1 + h0) + (1 - k_two) * (2 - h0))
    i0 = (1 - k_odd) * h0 + k_odd * (1 - k_two)
    own_lanes = pl.ds(pl.multiple_of(i0 * 128, 128), 128)
    put_out = [
        pltpu.make_async_copy(
            xg.at[g0, 2 * lax.rem(d0 + c, 2) + u, :, :, :, own_lanes],
            out.at[:, :, :, pl.ds(u * 128, 128)],
            loc.at[u],
        )
        for u in range(2)
    ]
    put_res = pltpu.make_async_copy(res, res_out, loc.at[2])
    spread_close(4)
    for cp in put_out:
        cp.start()
    predict(4)
    put_res.start()
    loss_s[...] = row_squares(res[...])
    stat_open("l", loss_s, loss_in)
    loss[...] = stat_take("l", loss_s, loss_in) / HT
    for cp in put_out:
        cp.wait()
    put_res.wait()
    for out_tag, ref in (
        ("w", w1.at[pl.ds(0, 7)]), ("m", w2.at[pl.ds(0, 7)]), ("p", pj.at[pl.ds(0, 7)]),
        ("t", ta.at[pl.ds(0, 7)]), ("sums0", part.at[pl.ds(0, 3)]), ("v1", sq), ("a", part.at[pl.ds(0, 6)]),
        ("b", r2), ("c", r2), ("d", xg.at[pl.ds(0, 3)]), ("q", stat_in), ("l", loss_in),
    ):
        net.flush(out_tag, ref)


def call_kernel(*args):
    vm = pl.BlockSpec(memory_space=pltpu.VMEM)
    hb = pl.BlockSpec(memory_space=pl.ANY)
    return pl.pallas_call(
        kernel,
        name="first",
        out_shape=(
            jax.ShapeDtypeStruct((4, 4, 32, 256), BF),
            jax.ShapeDtypeStruct((512, 512), F32),
            jax.ShapeDtypeStruct((1, 512), F32),
        ),
        in_specs=[vm, hb, vm, vm, vm, hb, hb, hb, hb, vm, vm],
        out_specs=(hb, hb, vm),
        scratch_shapes=[
            pltpu.VMEM((512, 512), F32),
            pltpu.VMEM((8, 2, 256, 1792), BF),
            pltpu.VMEM((4, 4, 4, 4, 32, 256), BF),
            pltpu.VMEM((4, 512, 512), BF),
            pltpu.VMEM((16, 4, 4, 32, 512), BF),
            pltpu.VMEM((4, 6, 4, 32, 512), BF),
            pltpu.VMEM((4, 6, 4, 32, 512), BF),
            pltpu.VMEM((3, 2, 4, 32, 512), BF),
            pltpu.VMEM((3, 2, 4, 32, 512), BF),
            pltpu.VMEM((3, 2, 4, 32, 512), BF),
            pltpu.VMEM((3, 2, 4, 32, 512), BF),
            pltpu.VMEM((512, 1792), F32),
            pltpu.VMEM((512, 896), BF),
            pltpu.VMEM((16, 32, 256), BF),
            pltpu.VMEM((8, 2, 896, 256), BF),
            pltpu.VMEM((8, 2, 256, 512), BF),
            pltpu.VMEM((4, 2, 3, 4, 32, 512), BF),
            pltpu.VMEM((4, 2, 3, 32, 512), BF),
            pltpu.VMEM((15, 8, 512), F32),
            pltpu.VMEM((8, 512), F32),
            pltpu.VMEM((15, 8, 512), F32),
            pltpu.VMEM((8, 512), F32),
            pltpu.VMEM((8, 512), F32),
            pltpu.VMEM((8, 128, 512), BF),
            pltpu.SemaphoreType.DMA((9,)),
            pltpu.SemaphoreType.DMA((4,)),
            pltpu.SemaphoreType.REGULAR,
            pltpu.SemaphoreType.DMA((SENDS,)),
            pltpu.SemaphoreType.DMA((RECEIVES,)),
        ],
        compiler_params=pltpu.CompilerParams(
            collective_id=0, has_side_effects=True, vmem_limit_bytes=67043328
        ),
    )(*args)


def keep(*refs):
    sources, results, held, sems = refs[0:3], refs[3:6], refs[6:9], refs[9]
    pieces = []
    for n, (a, v, o) in enumerate(zip(sources, held, results)):
        cuts = [slice(None)] if n else [pl.ds(i, 1) for i in range(4)]
        pieces += [(a.at[cut], v.at[cut], o.at[cut]) for cut in cuts]
    inward = [pltpu.make_async_copy(a, v, sems.at[i]) for i, (a, v, o) in enumerate(pieces)]
    outward = [pltpu.make_async_copy(v, o, sems.at[i]) for i, (a, v, o) in enumerate(pieces)]
    for cp in inward:
        cp.start()
    for before, after in zip(inward, outward):
        before.wait()
        after.start()
    for cp in outward:
        cp.wait()


def local(
    attn_ctx,
    w_out,
    resid,
    teacher_gain,
    dest_row,
    student_in,
    student_gain,
    w_gate,
    w_up,
    w_down,
    proj,
):
    out, residue, loss = call_kernel(
        attn_ctx,
        w_out,
        resid,
        student_in.reshape(4, 4, 32, 256),
        student_gain.reshape(32, 128),
        w_gate,
        w_up,
        w_down,
        proj,
        teacher_gain.reshape(64, 128),
        dest_row.reshape(16, 1, 256),
    )
    made = (residue.reshape(4, 128, 512), out.reshape(512, 256), loss)
    hb = pl.BlockSpec(memory_space=pl.ANY)
    residue, out, loss = pl.pallas_call(
        keep,
        name="keep",
        out_shape=tuple(jax.ShapeDtypeStruct(a.shape, a.dtype) for a in made),
        in_specs=[hb, hb, hb],
        out_specs=(hb, hb, hb),
        scratch_shapes=[pltpu.VMEM(a.shape, a.dtype) for a in made] + [pltpu.SemaphoreType.DMA((6,))],
    )(*made)
    return (out, loss.reshape(512), residue.reshape(512, 512))


def solution(mesh):
    torus = Mesh(mesh.devices.reshape(4, 2, 4, 4), AXES)
    in_specs = (
        P(DP, TENSOR),
        P(TENSOR, None),
        P(DP + TENSOR, None),
        P(),
        P(),
        P(DP, TENSOR),
        P(),
        P(DP, TENSOR),
        P(DP, TENSOR),
        P(TENSOR, DP),
        P(DP, TENSOR),
    )
    out_specs = (P(DP, TENSOR), P(DP), P(DP, TENSOR))
    return jax.shard_map(local, mesh=torus, in_specs=in_specs, out_specs=out_specs, check_vma=False)
```
